16 devices in a mesh: dp: 2 (over y, z), tp: 8 (over x, core).
Axes of the slice: x: 4, y: 2, z: 1, core: 2. Of those that a mesh axis runs over, the one named last changes fastest.
The devices are a block of a 4x4x8 slice.
Arguments:
- x: bfloat16 [4096, 5120], P(('dp', 'tp')), parts along dimension 0
- gain: bfloat16 [5120], replicated
- wq: bfloat16 [5120, 5120], P(None, 'tp')
- wk: bfloat16 [5120, 5120], P(None, 'tp')
- wv: bfloat16 [5120, 5120], P(None, 'tp')
- wo: bfloat16 [5120, 5120], P('tp')
Outputs:
- output: bfloat16 [4096, 5120], P(('dp', 'tp')), parts along dimension 0
There are 2 independent parts. The reference program is written for one: setup_inputs(seed, part) draws one part's arguments, and reference() takes and returns one part's arrays. A program takes and returns all parts, laid end to end along the dimension named above; an argument that names none is the same for every part.
All inputs are finite; a program needn't handle non-finite values.
Results may differ from the reference program's by a relative error of at most 0.012.
Values are sent between devices in bfloat16 or wider.
A program may use at most 768 MiB of HBM per device.

```python
import jax
import jax.numpy as jnp
from jax import lax

ROWS = 2048
D = 5120
HEADS = 40
KV_HEADS = 40
HEAD = 128
THETA = 10000


def setup_inputs(seed: int = 0, part: int = 0) -> dict:
    kx, kn, kq, kk, kv, ko = jax.random.split(jax.random.key(seed), 6)

    def weights(key, rows, columns):
        return jax.random.normal(key, (rows, columns), jnp.float32) * rows**-0.5

    drawn = {
        "x": jax.random.normal(jax.random.fold_in(kx, part), (ROWS, D), jnp.float32),
        "gain": 1 + 0.1 * jax.random.normal(kn, (D,), jnp.float32),
        "wq": 2 * weights(kq, D, HEADS * HEAD),
        "wk": 2 * weights(kk, D, KV_HEADS * HEAD),
        "wv": 4 * weights(kv, D, KV_HEADS * HEAD),
        "wo": weights(ko, HEADS * HEAD, D),
    }
    return {k: v.astype(jnp.bfloat16) for k, v in drawn.items()}


def normed(x, gain):
    wide = x.astype(jnp.float32)
    scale = lax.rsqrt(jnp.mean(wide * wide, -1, keepdims=True) + 1e-6)
    return (wide * scale * gain.astype(jnp.float32)).astype(jnp.bfloat16)


def turned(t, place, theta):
    half = t.shape[-1] // 2
    angle = place.astype(jnp.float32)[:, None] * theta ** (-jnp.arange(half, dtype=jnp.float32) / half)
    cos, sin = jnp.cos(angle)[:, None], jnp.sin(angle)[:, None]
    a, b = t[..., :half].astype(jnp.float32), t[..., half:].astype(jnp.float32)
    return jnp.concatenate([a * cos - b * sin, b * cos + a * sin], -1).astype(jnp.bfloat16)


def matmul(a, w):
    return jnp.dot(a, w, preferred_element_type=jnp.float32).astype(jnp.bfloat16)


def einsum(form, a, b):
    return jnp.einsum(form, a.astype(jnp.float32), b.astype(jnp.float32))


def attention(q, k, v):
    scores = einsum("tgsd,ugd->gstu", q, k) * q.shape[-1] ** -0.5
    token = jnp.arange(q.shape[0])
    scores = jnp.where(token[:, None] >= token, scores, -jnp.inf)
    weights = jax.nn.softmax(scores, -1).astype(jnp.bfloat16)
    return einsum("gstu,ugd->tgsd", weights, v).astype(jnp.bfloat16)


def reference(x, gain, wq, wk, wv, wo):
    a, place = normed(x, gain), jnp.arange(ROWS)
    q = turned(matmul(a, wq).reshape(ROWS, HEADS, HEAD), place, THETA).reshape(ROWS, KV_HEADS, -1, HEAD)
    k = turned(matmul(a, wk).reshape(ROWS, KV_HEADS, HEAD), place, THETA)
    v = matmul(a, wv).reshape(ROWS, KV_HEADS, HEAD)
    seen = attention(q, k, v).reshape(ROWS, HEADS * HEAD)
    return (x.astype(jnp.float32) + jnp.dot(seen, wo, preferred_element_type=jnp.float32)).astype(jnp.bfloat16)
```

```python
import functools

import jax
import jax.numpy as jnp
import numpy as np
from jax import lax
from jax.experimental import pallas as pl
from jax.experimental.pallas import tpu as pltpu
from jax.sharding import PartitionSpec as P

HEAD = 128
THETA = 10000
NEG = -1e30
HIDDEN = 2 * NEG
LOG2E = 1.4426950408889634
VMEM = 67_000_000
CHUNK = 512
MESH = pl.DeviceIdType.MESH


def _dot(a, b, ca, cb):
    return lax.dot_general(a, b, (((ca,), (cb,)), ((), ())), preferred_element_type=jnp.float32)


def _places(n):
    me = lax.axis_index("tp")
    chips = n // 2
    chip, core = me // 2, me % 2
    right = 2 * ((chip + 1) % chips) + core
    left = 2 * ((chip + chips - 1) % chips) + core
    return chip, core, left, right, 2 * chip + 1 - core


def _meet(devices):
    barrier = pltpu.get_barrier_semaphore()
    for d in devices:
        pl.semaphore_signal(barrier, inc=1, device_id={"tp": d}, device_id_type=MESH)
    pl.semaphore_wait(barrier, len(devices))


def _send(src, dst, send_sem, recv_sem, device):
    return pltpu.make_async_remote_copy(src_ref=src, dst_ref=dst, send_sem=send_sem, recv_sem=recv_sem, device_id={"tp": device}, device_id_type=MESH)


def gather_project(n, x_ref, gain_ref, near_ref, far_ref, wq_hbm, wk_hbm, wv_hbm, q_ref, k_ref, v_ref, held, w, w_sem,
                   send_r, send_l, send_p, recv_r, recv_l, recv_p):
    chip, core, left, right, partner = _places(n)
    chips = n // 2
    rows, cols = x_ref.shape
    width = wq_hbm.shape[1]
    heads = width // HEAD
    piece = rows // 4

    loads = [pltpu.make_async_copy(src, w.at[:, pl.ds(i * width, width)], w_sem.at[i]) for i, src in enumerate((wq_hbm, wk_hbm, wv_hbm))]
    for load in loads:
        load.start()
    _meet((left, right, partner))

    def at(i):
        return pl.ds(i * piece, piece)

    def to_right(src, s):
        return _send(src, held.at[s + 1, at(0)], send_r.at[s - 1], recv_l.at[s - 1], right)

    def to_left(src, s):
        return _send(src, held.at[s + 1, at(1)], send_l.at[s - 1], recv_r.at[s - 1], left)

    def to_partner(s):
        if isinstance(s, int) and s == 0:
            return _send(held.at[0], held.at[1], send_p.at[0], recv_p.at[0], partner)
        return _send(held.at[s + 1, pl.ds(0, 2 * piece)], held.at[s + 1, pl.ds(2 * piece, 2 * piece)], send_p.at[s], recv_p.at[s], partner)

    gain = gain_ref[...].astype(jnp.float32)

    def norm(i):
        wide = x_ref[i * piece : (i + 1) * piece, :].astype(jnp.float32)
        scale = lax.rsqrt(jnp.mean(wide * wide, -1, keepdims=True) + 1e-6)
        held[0, i * piece : (i + 1) * piece, :] = (wide * scale * gain).astype(jnp.bfloat16)

    norm(0)
    norm(2)
    to_right(held.at[0, at(0)], 1).start()
    norm(1)
    to_left(held.at[0, at(2)], 1).start()
    norm(3)
    to_right(held.at[0, at(1)], 2).start()
    to_left(held.at[0, at(3)], 2).start()
    to_partner(0).start()
    to_right(held.at[0, at(2)], 3).start()
    to_left(held.at[0, at(0)], 3).start()
    to_right(held.at[0, at(3)], 4).start()
    to_left(held.at[0, at(1)], 4).start()
    for load in loads:
        load.wait()

    first_half = lax.broadcasted_iota(jnp.int32, (1, HEAD), 1) < HEAD // 2
    outs = (q_ref, k_ref, v_ref)

    def project(slot, starts):
        turns = []
        for start in starts:
            j = start // piece
            c, s = far_ref[0, pl.ds(j, 1), :], far_ref[1, pl.ds(j, 1), :]
            cn, sn = near_ref[0], near_ref[1]
            turns.append((c * cn - s * sn, jnp.where(first_half, -1.0, 1.0) * (s * cn + c * sn)))
        cos = jnp.concatenate([t[0] for t in turns], axis=0)
        sin = jnp.concatenate([t[1] for t in turns], axis=0)
        for h0 in range(0, 3 * heads, 4):
            got = list(range(h0, min(h0 + 4, 3 * heads)))
            t = _dot(held[slot], w[:, h0 * HEAD : (got[-1] + 1) * HEAD], 1, 0).astype(jnp.bfloat16)
            for h in got:
                th = t[:, (h - h0) * HEAD : (h - h0 + 1) * HEAD]
                if h < 2 * heads:
                    wide = th.astype(jnp.float32)
                    th = (wide * cos + pltpu.roll(wide, HEAD // 2, 1) * sin).astype(jnp.bfloat16)
                for i, start in enumerate(starts):
                    outs[h // heads][h % heads, pl.ds(pl.multiple_of(start, piece), piece), :] = th[i * piece : (i + 1) * piece, :]

    def step(s, _):
        t = s - 1

        @pl.when(s == 1)
        def _():
            to_partner(0).wait_recv()

        @pl.when(s >= 2)
        def _():
            to_right(held.at[0, at(0)], t).wait_recv()
            to_left(held.at[0, at(0)], t).wait_recv()
            to_partner(t).start()

            @pl.when(t <= 2)
            def _():
                to_right(held.at[t + 1, at(0)], t + 4).start()
                to_left(held.at[t + 1, at(1)], t + 4).start()

            to_partner(t).wait_recv()

        late = t > 4
        l_chip = (chip + chips - jnp.where(late, 2, 1)) % chips
        r_chip = (chip + jnp.where(late, 2, 1)) % chips
        l_piece = jnp.where(late, t - 5, t - 1)
        r_piece = jnp.where(late, t - 3, (t + 1) % 4)
        starts = []
        for i in range(4):
            c = core if i < 2 else 1 - core
            landed = (l_chip, l_piece) if i % 2 == 0 else (r_chip, r_piece)
            landed_at = (2 * landed[0] + c) * rows + landed[1] * piece
            whole_at = (2 * chip + jnp.where(s == 0, core, 1 - core)) * rows + i * piece
            starts.append(jnp.where(s < 2, whole_at, landed_at))
        project(s, starts)
        return _

    lax.fori_loop(0, 8, step, None)

    for s in range(1, 7):
        to_right(held.at[0, at(0)], s).wait_send()
        to_left(held.at[0, at(0)], s).wait_send()
    for s in range(7):
        to_partner(s).wait_send()


def _tables(rows, piece, count):
    half = HEAD // 2
    step = float(THETA) ** (-np.arange(half, dtype=np.float64) / half)

    def pair(place):
        angle = place[:, None] * np.concatenate([step, step])[None, :]
        return np.stack([np.cos(angle), np.sin(angle)]).astype(np.float32)

    return pair(np.arange(piece, dtype=np.float64)), pair(piece * np.arange(count, dtype=np.float64))


def projected(n, x, gain, wq, wk, wv):
    rows, cols = x.shape
    width = wq.shape[1]
    heads = width // HEAD
    tokens = n * rows
    near, far = _tables(rows, rows // 4, tokens // (rows // 4))
    vmem, hbm = pl.BlockSpec(memory_space=pltpu.VMEM), pl.BlockSpec(memory_space=pl.ANY)
    out = jax.ShapeDtypeStruct((heads, tokens, HEAD), jnp.bfloat16)
    dma = pltpu.SemaphoreType.DMA
    return pl.pallas_call(
        functools.partial(gather_project, n),
        name="gather_project",
        out_shape=[out] * 3,
        in_specs=[vmem] * 4 + [hbm] * 3,
        out_specs=[vmem] * 3,
        scratch_shapes=[
            pltpu.VMEM((8, rows, cols), jnp.bfloat16),
            pltpu.VMEM((cols, 3 * width), jnp.bfloat16),
            dma((3,)), dma((6,)), dma((6,)), dma((7,)), dma((6,)), dma((6,)), dma((7,)),
        ],
        compiler_params=pltpu.CompilerParams(collective_id=0, has_side_effects=True, vmem_limit_bytes=VMEM),
    )(x, gain.reshape(1, cols), jnp.asarray(near), jnp.asarray(far), wq, wk, wv)


def attend_scatter(n, x_ref, q_ref, k_ref, v_ref, wo_ref, y_hbm, seen, top_s, mix_s, give, sum_r, sum_l, y_s, from_p, from_l, from_r,
                   give_sem, give_got, send_r, send_l, got_l, got_r, y_sem):
    chip, core, left, right, partner = _places(n)
    chips = n // 2
    rows, cols = x_ref.shape
    heads = q_ref.shape[0]
    count = cols // CHUNK
    half = count // 2
    e = HEAD**-0.5 * LOG2E
    _meet((left, right, partner))

    def columns(j):
        return pl.ds(pl.multiple_of(j * CHUNK, CHUNK), CHUNK)

    hidden = lax.broadcasted_iota(jnp.int32, (rows, rows), 0) > lax.broadcasted_iota(jnp.int32, (rows, rows), 1)
    ones = jnp.ones((8, rows), jnp.bfloat16)

    def attend(chip_to, core_to, slot):
        block_to = 2 * chip_to + core_to
        here = pl.ds(pl.multiple_of(block_to * rows, rows), rows)
        top_s[...] = jnp.full(top_s.shape, NEG, jnp.float32)
        mix_s[...] = jnp.zeros(mix_s.shape, jnp.float32)

        def block(j, masked):
            keys = pl.ds(pl.multiple_of(j * rows, rows), rows)
            scores = [_dot(k_ref[h, keys, :], q_ref[h, here, :], 1, 1) for h in range(heads)]
            weights, keeps = [], []
            for h, s in enumerate(scores):
                if masked:
                    s = jnp.where(hidden, HIDDEN, s)
                old = top_s[h : h + 1, :]
                top = jnp.maximum(old, s.max(axis=0, keepdims=True))
                top_s[h : h + 1, :] = top
                weights.append(jnp.exp2((s - top) * e).astype(jnp.bfloat16))
                keeps.append(jnp.exp2((old - top) * e))
            for h, (p, keep) in enumerate(zip(weights, keeps)):
                values = jnp.concatenate([v_ref[h, keys, :].T, ones], axis=0)
                mix_s[h] = mix_s[h] * keep + _dot(values, p, 1, 0)

        lax.fori_loop(0, block_to, lambda j, _: block(j, False), None)
        block(block_to, True)
        for h in range(heads):
            o = mix_s[h, :HEAD, :] * (1 / mix_s[h, HEAD : HEAD + 1, :])
            seen[slot, :, h * HEAD : (h + 1) * HEAD] = o.T.astype(jnp.bfloat16)

    def term(slot, j):
        return _dot(seen[slot], wo_ref[:, columns(j)], 1, 0)

    def give_copy(g, j):
        return _send(give.at[g % 2, j], from_p.at[g, j], give_sem.at[g, j], give_got.at[g, j], partner)

    def to_right(slot):
        return _send(sum_r.at[slot], from_l.at[slot], send_r.at[slot], got_l.at[slot], right)

    def to_left(slot):
        return _send(sum_l.at[slot], from_r.at[slot], send_l.at[slot], got_r.at[slot], left)

    def hand_over(g, chip_to):
        attend(chip_to, 1 - core, 0)

        def body(i, _):
            j = i // 2 + (i % 2) * half
            if g >= 2:
                give_copy(g - 2, j).wait_send()
            give[g % 2, j] = term(0, j).astype(jnp.bfloat16)
            give_copy(g, j).start()
            return _

        lax.fori_loop(0, count, body, None)

    def pair(g, slot, j):
        give_copy(g, j).wait_recv()
        return term(slot, j) + from_p[g, j].astype(jnp.float32)

    def emit_right(slot, value):
        sum_r[slot] = value.astype(jnp.bfloat16)
        to_right(slot).start()

    def emit_left(slot, value):
        sum_l[slot] = value.astype(jnp.bfloat16)
        to_left(slot).start()

    def loop(body):
        def run(j, _):
            body(j)
            return _

        lax.fori_loop(0, half, run, None)

    across, after, before = (chip + 2) % chips, (chip + 1) % chips, (chip + chips - 1) % chips

    hand_over(0, across)
    attend(across, core, 0)

    def first(j):
        emit_right(j, pair(0, 0, j))
        emit_left(j, pair(0, 0, half + j))

    loop(first)
    hand_over(1, after)
    attend(after, core, 1)
    loop(lambda j: emit_right(2 * half + j, pair(1, 1, half + j)))
    hand_over(2, before)
    attend(before, core, 2)
    loop(lambda j: emit_left(half + j, pair(2, 2, j)))
    hand_over(3, chip)
    attend(chip, core, 3)

    def second(j):
        to_right(j).wait_recv()
        emit_right(half + j, pair(1, 1, j) + from_l[j].astype(jnp.float32))
        to_left(j).wait_recv()
        emit_left(2 * half + j, pair(2, 2, half + j) + from_r[j].astype(jnp.float32))

    loop(second)

    def y_copy(j):
        return pltpu.make_async_copy(y_s.at[j], y_hbm.at[:, columns(j)], y_sem.at[j])

    def last(j):
        to_right(half + j).wait_recv()
        to_left(half + j).wait_recv()
        total = pair(3, 3, j) + from_l[half + j].astype(jnp.float32) + from_r[half + j].astype(jnp.float32)
        y_s[j] = (x_ref[:, columns(j)].astype(jnp.float32) + total).astype(jnp.bfloat16)
        y_copy(j).start()

    def both(j):
        last(j)
        last(half + j)

    loop(both)

    def drain(i, _):
        give_copy(2, i).wait_send()
        give_copy(3, i).wait_send()
        y_copy(i).wait()
        return _

    lax.fori_loop(0, count, drain, None)

    def drain_ring(i, _):
        to_right(i).wait_send()
        to_left(i).wait_send()
        return _

    lax.fori_loop(0, half + count, drain_ring, None)


def attended(n, x, q, k, v, wo):
    rows, cols = x.shape
    heads = q.shape[0]
    count = cols // CHUNK
    ring = count + count // 2
    vmem, hbm = pl.BlockSpec(memory_space=pltpu.VMEM), pl.BlockSpec(memory_space=pl.ANY)
    dma = pltpu.SemaphoreType.DMA

    def chunks(*lead):
        return pltpu.VMEM((*lead, rows, CHUNK), jnp.bfloat16)

    return pl.pallas_call(
        functools.partial(attend_scatter, n),
        name="attend_scatter",
        out_shape=jax.ShapeDtypeStruct((rows, cols), jnp.bfloat16),
        in_specs=[vmem] * 5,
        out_specs=hbm,
        scratch_shapes=[
            pltpu.VMEM((4, rows, heads * HEAD), jnp.bfloat16),
            pltpu.VMEM((heads, rows), jnp.float32),
            pltpu.VMEM((heads, HEAD + 8, rows), jnp.float32),
            chunks(2, count), chunks(ring), chunks(ring), chunks(count), chunks(4, count), chunks(ring), chunks(ring),
            dma((4, count)), dma((4, count)), dma((ring,)), dma((ring,)), dma((ring,)), dma((ring,)), dma((count,)),
        ],
        compiler_params=pltpu.CompilerParams(collective_id=1, has_side_effects=True, vmem_limit_bytes=VMEM),
    )(x, q, k, v, wo)


def solution(mesh):
    n = mesh.shape["tp"]

    def step(x, gain, wq, wk, wv, wo):
        q, k, v = projected(n, x, gain, wq, wk, wv)
        return attended(n, x, q, k, v, wo)

    tokens, columns = P(("dp", "tp"), None), P(None, "tp")
    return jax.shard_map(
        step,
        mesh=mesh,
        in_specs=(tokens, P(None), columns, columns, columns, P("tp", None)),
        out_specs=tokens,
        check_vma=False,
    )
```

```python
import functools

import jax
import jax.numpy as jnp
import numpy as np
from jax import lax
from jax.experimental import pallas as pl
from jax.experimental.pallas import tpu as pltpu
from jax.sharding import PartitionSpec as P

HEAD = 128
THETA = 10000
NEG = -1e30
HIDDEN = 2 * NEG
LOG2E = 1.4426950408889634
VMEM = 67_043_328
CHUNK = 512
MESH = pl.DeviceIdType.MESH


def _dot(a, b, ca, cb):
    return lax.dot_general(a, b, (((ca,), (cb,)), ((), ())), preferred_element_type=jnp.float32)


def _places(n):
    me = lax.axis_index("tp")
    chips = n // 2
    chip, core = me // 2, me % 2
    right = 2 * ((chip + 1) % chips) + core
    left = 2 * ((chip + chips - 1) % chips) + core
    return chip, core, left, right, 2 * chip + 1 - core


def _meet(devices):
    barrier = pltpu.get_barrier_semaphore()
    for d in devices:
        pl.semaphore_signal(barrier, inc=1, device_id={"tp": d}, device_id_type=MESH)
    pl.semaphore_wait(barrier, len(devices))


def _send(src, dst, send_sem, recv_sem, device):
    return pltpu.make_async_remote_copy(src_ref=src, dst_ref=dst, send_sem=send_sem, recv_sem=recv_sem, device_id={"tp": device}, device_id_type=MESH)


def _tables(rows, piece, count):
    half = HEAD // 2
    step = float(THETA) ** (-np.arange(half, dtype=np.float64) / half)

    def pair(place):
        angle = place[:, None] * np.concatenate([step, step])[None, :]
        return np.stack([np.cos(angle), np.sin(angle)]).astype(np.float32)

    return pair(np.arange(piece, dtype=np.float64)), pair(piece * np.arange(count, dtype=np.float64))


def layer(n, x_hbm, gain_ref, near_ref, far_ref, wq_hbm, wk_hbm, wv_hbm, wo_hbm, y_hbm, x_s, held, w, wo, q_s, k_s, v_s, seen, top_s, mix_s,
          x_sem, w_sem, send_r, send_l, send_p, recv_r, recv_l, recv_p, give_sem, give_got, sum_r_sem, sum_l_sem, got_l, got_r, y_sem, ready1, ready2):
    chip, core, left, right, partner = _places(n)
    chips = n // 2
    rows, cols = x_s.shape
    heads = q_s.shape[0]
    width = heads * HEAD
    piece = rows // 4
    count = cols // CHUNK
    half = count // 2
    e = HEAD**-0.5 * LOG2E
    across, after, before = (chip + 2) % chips, (chip + 1) % chips, (chip + chips - 1) % chips

    x_loads = [pltpu.make_async_copy(x_hbm.at[pl.ds(i * piece, piece)], x_s.at[pl.ds(i * piece, piece)], x_sem.at[i]) for i in range(4)]
    for load in x_loads:
        load.start()
    loads = [pltpu.make_async_copy(src, w.at[:, pl.ds(i * width, width)], w_sem.at[i]) for i, src in enumerate((wq_hbm, wk_hbm, wv_hbm))]
    loads.append(pltpu.make_async_copy(wo_hbm, wo, w_sem.at[3]))
    for load in loads:
        load.start()
    _meet((left, right, partner))


    def at(i):
        return pl.ds(i * piece, piece)

    def to_right(src, s):
        return _send(src, held.at[s + 1, :, at(0)], send_r.at[s - 1], recv_l.at[s - 1], right)

    def to_left(src, s):
        return _send(src, held.at[s + 1, :, at(1)], send_l.at[s - 1], recv_r.at[s - 1], left)

    def to_partner(s):
        if isinstance(s, int) and s == 0:
            return _send(held.at[0], held.at[1], send_p.at[0], recv_p.at[0], partner)
        return _send(held.at[s + 1, :, pl.ds(0, 2 * piece)], held.at[s + 1, :, pl.ds(2 * piece, 2 * piece)], send_p.at[s], recv_p.at[s], partner)

    def own(i):
        return held.at[0, :, at(i)]

    gain = gain_ref[...].astype(jnp.float32).reshape(1, cols)

    def norm(i):
        x_loads[i].wait()
        wide = x_s[i * piece : (i + 1) * piece, :].astype(jnp.float32)
        scale = lax.rsqrt(jnp.mean(wide * wide, -1, keepdims=True) + 1e-6)
        a = (wide * scale * gain).astype(jnp.bfloat16)
        for c in range(count):
            held[0, c, i * piece : (i + 1) * piece, :] = a[:, c * CHUNK : (c + 1) * CHUNK]

    norm(0)
    norm(2)
    to_right(own(0), 1).start()
    norm(1)
    to_left(own(2), 1).start()
    norm(3)
    to_right(own(1), 2).start()
    to_left(own(3), 2).start()
    to_partner(0).start()
    to_right(own(2), 3).start()
    to_left(own(0), 3).start()
    to_right(own(3), 4).start()
    to_left(own(1), 4).start()
    for load in loads:
        load.wait()

    first_half = lax.broadcasted_iota(jnp.int32, (1, HEAD), 1) < HEAD // 2
    outs = (q_s, k_s, v_s)

    def project(slot, starts):
        turns = []
        for start in starts:
            j = start // piece
            c, s = far_ref[0, pl.ds(j, 1), :], far_ref[1, pl.ds(j, 1), :]
            cn, sn = near_ref[0], near_ref[1]
            turns.append((c * cn - s * sn, jnp.where(first_half, -1.0, 1.0) * (s * cn + c * sn)))
        cos = jnp.concatenate([t[0] for t in turns], axis=0)
        sin = jnp.concatenate([t[1] for t in turns], axis=0)
        for h0 in range(0, 3 * heads, 4):
            got = list(range(h0, min(h0 + 4, 3 * heads)))
            a = jnp.concatenate([held[slot, c] for c in range(count)], axis=1)
            t = _dot(a, w[:, h0 * HEAD : (got[-1] + 1) * HEAD], 1, 0).astype(jnp.bfloat16)
            for h in got:
                th = t[:, (h - h0) * HEAD : (h - h0 + 1) * HEAD]
                if h < 2 * heads:
                    wide = th.astype(jnp.float32)
                    th = (wide * cos + pltpu.roll(wide, HEAD // 2, 1) * sin).astype(jnp.bfloat16)
                for i, start in enumerate(starts):
                    outs[h // heads][h % heads, pl.ds(pl.multiple_of(start, piece), piece), :] = th[i * piece : (i + 1) * piece, :]

    def step(s, _):
        t = s - 1

        @pl.when(s == 1)
        def _():
            to_partner(0).wait_recv()

        @pl.when(s >= 2)
        def _():
            to_right(own(0), t).wait_recv()
            to_left(own(0), t).wait_recv()
            to_partner(t).start()

            @pl.when(t <= 2)
            def _():
                to_right(held.at[t + 1, :, at(0)], t + 4).start()
                to_left(held.at[t + 1, :, at(1)], t + 4).start()

            to_partner(t).wait_recv()

        late = t > 4
        l_chip, r_chip = jnp.where(late, across, before), jnp.where(late, across, after)
        l_piece = jnp.where(late, t - 5, t - 1)
        r_piece = jnp.where(late, t - 3, (t + 1) % 4)
        starts = []
        for i in range(4):
            c = core if i < 2 else 1 - core
            landed = (l_chip, l_piece) if i % 2 == 0 else (r_chip, r_piece)
            landed_at = (2 * landed[0] + c) * rows + landed[1] * piece
            whole_at = (2 * chip + jnp.where(s == 0, core, 1 - core)) * rows + i * piece
            starts.append(jnp.where(s < 2, whole_at, landed_at))
        project(s, starts)

        @pl.when(s == 5)
        def _():
            for u in range(1, 5):
                to_right(own(0), u).wait_send()
                to_left(own(0), u).wait_send()
            for u in range(5):
                to_partner(u).wait_send()
            for d in (left, right, partner):
                pl.semaphore_signal(ready1, inc=1, device_id={"tp": d}, device_id_type=MESH)
            lax.fori_loop(0, 4, lambda u, _: start_unit(u), None)

        return _


    hidden = lax.broadcasted_iota(jnp.int32, (rows, rows), 0) > lax.broadcasted_iota(jnp.int32, (rows, rows), 1)
    ones = jnp.ones((8, rows), jnp.bfloat16)

    def block(u, to, j, masked):
        here = pl.ds(pl.multiple_of(to * rows, rows), rows)
        keys = pl.ds(pl.multiple_of(j * rows, rows), rows)
        scores = [_dot(k_s[h, keys, :], q_s[h, here, :], 1, 1) for h in range(heads)]
        weights, keeps = [], []
        for h, s in enumerate(scores):
            if masked:
                s = jnp.where(hidden, HIDDEN, s)
            old = top_s[u, h : h + 1, :]
            top = jnp.maximum(old, s.max(axis=0, keepdims=True))
            top_s[u, h : h + 1, :] = top
            weights.append(jnp.exp2((s - top) * e).astype(jnp.bfloat16))
            keeps.append(jnp.exp2((old - top) * e))
        for h, (p, keep) in enumerate(zip(weights, keeps)):
            values = jnp.concatenate([v_s[h, keys, :].T, ones], axis=0)
            mix_s[u, h] = mix_s[u, h] * keep + _dot(values, p, 1, 0)

    def blocks(u, to, low, high):
        def run(j, _):
            block(u, to, j, False)
            return _

        lax.fori_loop(low, high, run, None)

    def clear(u):
        top_s[u] = jnp.full(top_s.shape[1:], NEG, jnp.float32)
        mix_s[u] = jnp.zeros(mix_s.shape[1:], jnp.float32)

    def unit(u):
        to_chip = jnp.where(u < 2, after, before)
        return to_chip, 2 * to_chip + jnp.where(u % 2 == 0, 1 - core, core)

    def start_unit(u):
        to_chip, to = unit(u)
        clear(u)
        blocks(u, to, 0, jnp.minimum(2 * across, to))
        blocks(u, to, 2 * across + 2, to)
        block(u, to, to, True)

    def finish(u, slot):
        for h in range(heads):
            o = mix_s[u, h, :HEAD, :] * (1 / mix_s[u, h, HEAD : HEAD + 1, :])
            seen[slot, :, h * HEAD : (h + 1) * HEAD] = o.T.astype(jnp.bfloat16)

    def finish_unit(u):
        to_chip, to = unit(u)
        blocks(u, to, 2 * across, 2 * across + jnp.where(across < to_chip, 2, 0))
        finish(u, u)

    def attend(to, slot):
        clear(0)
        blocks(0, to, 0, to)
        block(0, to, to, True)
        finish(0, slot)

    lax.fori_loop(0, 8, step, None)

    for s in (5, 6):
        to_right(own(0), s).wait_send()
        to_left(own(0), s).wait_send()
        to_partner(s).wait_send()
    for d in (left, right, partner):
        pl.semaphore_signal(ready2, inc=1, device_id={"tp": d}, device_id_type=MESH)


    def columns(j):
        return pl.ds(pl.multiple_of(j * CHUNK, CHUNK), CHUNK)

    def spare(i):
        return w.at[pl.ds(pl.multiple_of((i // 3) * rows, rows), rows), columns(i % 3)]

    sums = 3 * half
    out_right, out_left, give_at, y_at = 0, sums, 2 * sums, 2 * sums + 2 * count

    from_p_slots = (3, 0, 1, 6)

    def term(slot, j):
        return _dot(seen[slot], wo[:, columns(j)], 1, 0)

    def give_copy(g, j):
        return _send(spare(give_at + (g // 2 if g in (0, 3) else g - 1) * count + j), held.at[from_p_slots[g], j], give_sem.at[g, j],
                     give_got.at[g, j], partner)

    def ring_slot(base, part, j):
        return held.at[base, part * half + j] if part < 2 else held.at[2, (base - 4) * half + j]

    def right_copy(part, j):
        i = part * half + j
        return _send(spare(out_right + i), ring_slot(4, part, j), sum_r_sem.at[i], got_l.at[i], right)

    def left_copy(part, j):
        i = part * half + j
        return _send(spare(out_left + i), ring_slot(5, part, j), sum_l_sem.at[i], got_r.at[i], left)

    def landed_l(part, j):
        right_copy(part, j).wait_recv()
        return ring_slot(4, part, j)[...].astype(jnp.float32)

    def landed_r(part, j):
        left_copy(part, j).wait_recv()
        return ring_slot(5, part, j)[...].astype(jnp.float32)

    def give(g, slot, j):
        if g in (0, 3):
            give_copy(g // 3 + 1, j).wait_send()
        spare(give_at + (g // 2 if g in (0, 3) else g - 1) * count + j)[...] = term(slot, j).astype(jnp.bfloat16)
        give_copy(g, j).start()

    def pair(g, slot, j):
        give_copy(g, j).wait_recv()
        return term(slot, j) + held[from_p_slots[g], j].astype(jnp.float32)

    def emit_right(part, j, value):
        spare(out_right + part * half + j)[...] = value.astype(jnp.bfloat16)
        right_copy(part, j).start()

    def emit_left(part, j, value):
        spare(out_left + part * half + j)[...] = value.astype(jnp.bfloat16)
        left_copy(part, j).start()

    def loop(body):
        def run(j, _):
            body(j)
            return _

        lax.fori_loop(0, half, run, None)

    pl.semaphore_wait(ready1, 3)

    finish_unit(0)
    finish_unit(2)

    def begin(j):
        give(1, 0, half + j)
        give(2, 2, j)

    loop(begin)
    finish_unit(1)
    finish_unit(3)

    def part0(j):
        emit_right(0, j, pair(1, 1, half + j))
        emit_left(0, j, pair(2, 3, j))

    loop(part0)

    def rest(j):
        give(1, 0, j)
        give(2, 2, half + j)

    loop(rest)

    pl.semaphore_wait(ready2, 3)
    attend(2 * across + 1 - core, 0)

    def give_across(j):
        give(0, 0, j)
        give(0, 0, half + j)

    loop(give_across)
    attend(2 * across + core, 2)

    def part1(j):
        emit_right(1, j, pair(0, 2, j))
        emit_left(1, j, pair(0, 2, half + j))

    loop(part1)

    attend(2 * chip + 1 - core, 0)

    def give_own(j):
        give(3, 0, j)
        give(3, 0, half + j)

    loop(give_own)
    attend(2 * chip + core, 2)

    def part2(j):
        emit_right(2, j, pair(1, 1, j) + landed_l(1, j))
        emit_left(2, j, pair(2, 3, half + j) + landed_r(1, j))

    loop(part2)

    def y_copy(j):
        return pltpu.make_async_copy(spare(y_at + j), y_hbm.at[:, columns(j)], y_sem.at[j])

    def last(j, a, b):
        total = pair(3, 2, j) + a + b
        spare(y_at + j)[...] = (x_s[:, columns(j)].astype(jnp.float32) + total).astype(jnp.bfloat16)
        y_copy(j).start()

    def both(j):
        last(j, landed_l(2, j), landed_r(0, j))
        last(half + j, landed_l(0, j), landed_r(2, j))

    loop(both)

    def drain(i, _):
        give_copy(0, i).wait_send()
        give_copy(3, i).wait_send()
        y_copy(i).wait()
        return _

    lax.fori_loop(0, count, drain, None)

    def drain_ring(j):
        for part in range(3):
            right_copy(part, j).wait_send()
            left_copy(part, j).wait_send()

    loop(drain_ring)


def solution(mesh):
    n = mesh.shape["tp"]

    def step(x, gain, wq, wk, wv, wo):
        rows, cols = x.shape
        width = wq.shape[1]
        heads = width // HEAD
        tokens = n * rows
        count = cols // CHUNK
        ring = 3 * (count // 2)
        near, far = _tables(rows, rows // 4, tokens // (rows // 4))
        vmem, hbm = pl.BlockSpec(memory_space=pltpu.VMEM), pl.BlockSpec(memory_space=pl.ANY)
        dma = pltpu.SemaphoreType.DMA
        low = jnp.bfloat16
        return pl.pallas_call(
            functools.partial(layer, n),
            name="layer",
            out_shape=jax.ShapeDtypeStruct((rows, cols), low),
            in_specs=[hbm] + [vmem] * 3 + [hbm] * 4,
            out_specs=hbm,
            scratch_shapes=[
                pltpu.VMEM((rows, cols), low),
                pltpu.VMEM((8, count, rows, CHUNK), low),
                pltpu.VMEM((cols, 3 * width), low),
                pltpu.VMEM((width, cols), low),
                *[pltpu.VMEM((heads, tokens, HEAD), low)] * 3,
                pltpu.VMEM((4, rows, width), low),
                pltpu.VMEM((4, heads, rows), jnp.float32),
                pltpu.VMEM((4, heads, HEAD + 8, rows), jnp.float32),
                dma((4,)), dma((4,)), dma((6,)), dma((6,)), dma((7,)), dma((6,)), dma((6,)), dma((7,)),
                dma((4, count)), dma((4, count)), dma((ring,)), dma((ring,)), dma((ring,)), dma((ring,)), dma((count,)),
                pltpu.SemaphoreType.REGULAR, pltpu.SemaphoreType.REGULAR,
            ],
            compiler_params=pltpu.CompilerParams(collective_id=0, has_side_effects=True, vmem_limit_bytes=VMEM),
        )(x, gain, jnp.asarray(near), jnp.asarray(far), wq, wk, wv, wo)

    tokens, columns = P(("dp", "tp"), None), P(None, "tp")
    return jax.shard_map(
        step,
        mesh=mesh,
        in_specs=(tokens, P(None), columns, columns, columns, P("tp", None)),
        out_specs=tokens,
        check_vma=False,
    )
```

```python
import functools

import jax
import jax.numpy as jnp
import numpy as np
from jax import lax
from jax.experimental import pallas as pl
from jax.experimental.pallas import tpu as pltpu
from jax.sharding import PartitionSpec as P

HEAD = 128
THETA = 10000
NEG = -1e30
HIDDEN = 2 * NEG
LOG2E = 1.4426950408889634
VMEM = 67_043_328
CHUNK = 512
MESH = pl.DeviceIdType.MESH


def _dot(a, b, ca, cb):
    return lax.dot_general(a, b, (((ca,), (cb,)), ((), ())), preferred_element_type=jnp.float32)


def _places(n):
    me = lax.axis_index("tp")
    chips = n // 2
    chip, core = me // 2, me % 2
    right = 2 * ((chip + 1) % chips) + core
    left = 2 * ((chip + chips - 1) % chips) + core
    return chip, core, left, right, 2 * chip + 1 - core


def _meet(devices):
    barrier = pltpu.get_barrier_semaphore()
    for d in devices:
        pl.semaphore_signal(barrier, inc=1, device_id={"tp": d}, device_id_type=MESH)
    pl.semaphore_wait(barrier, len(devices))


def _send(src, dst, send_sem, recv_sem, device):
    return pltpu.make_async_remote_copy(src_ref=src, dst_ref=dst, send_sem=send_sem, recv_sem=recv_sem, device_id={"tp": device}, device_id_type=MESH)


def _tables(rows, piece, count):
    half = HEAD // 2
    step = float(THETA) ** (-np.arange(half, dtype=np.float64) / half)

    def pair(place):
        angle = place[:, None] * np.concatenate([step, step])[None, :]
        return np.stack([np.cos(angle), np.sin(angle)]).astype(np.float32)

    return pair(np.arange(piece, dtype=np.float64)), pair(piece * np.arange(count, dtype=np.float64))


def layer(n, x_hbm, gain_ref, near_ref, far_ref, wq_hbm, wk_hbm, wv_hbm, wo_hbm, y_hbm, x_s, held, w, wo, q_s, k_s, v_s, seen, top_s, mix_s,
          x_sem, w_sem, send_r, send_l, send_p, recv_r, recv_l, recv_p, give_sem, give_got, sum_r_sem, sum_l_sem, got_l, got_r, y_sem, ready1, ready2, ready3):
    chip, core, left, right, partner = _places(n)
    chips = n // 2
    rows, cols = x_s.shape
    heads = q_s.shape[0]
    width = heads * HEAD
    piece, short = rows // 4, rows // 8
    count = cols // CHUNK
    half = count // 2
    e = HEAD**-0.5 * LOG2E
    across, after, before = (chip + 2) % chips, (chip + 1) % chips, (chip + chips - 1) % chips

    x_loads = [pltpu.make_async_copy(x_hbm.at[pl.ds(i * piece, piece)], x_s.at[pl.ds(i * piece, piece)], x_sem.at[i]) for i in range(4)]
    for load in x_loads:
        load.start()
    _meet((left, right, partner))
    loads = [pltpu.make_async_copy(src, w.at[:, pl.ds(i * width, width)], w_sem.at[i]) for i, src in enumerate((wk_hbm, wv_hbm, wq_hbm))]
    loads.append(pltpu.make_async_copy(wo_hbm, wo, w_sem.at[3]))


    def at(i):
        return pl.ds(i * piece, piece)

    def lands(s, quarter, quarters=1):
        if isinstance(s, int) and s < 5:
            return held.at[s + 1, :, pl.ds(quarter * piece, quarters * piece)]
        return held.at[6 + (s - 5) // 2, :, pl.ds(pl.multiple_of((s - 5) % 2 * 2 * piece + quarter * short, short), quarters * short)]

    def long_lands(s, quarter, quarters=1):
        return held.at[s + 1, :, pl.ds(quarter * piece, quarters * piece)]

    def to_right(src, s, to=lands):
        return _send(src, to(s, 0), send_r.at[s - 1], recv_l.at[s - 1], right)

    def to_left(src, s, to=lands):
        return _send(src, to(s, 1), send_l.at[s - 1], recv_r.at[s - 1], left)

    def to_partner(s, to=lands):
        if isinstance(s, int) and s == 0:
            return _send(held.at[0], held.at[1], send_p.at[0], recv_p.at[0], partner)
        return _send(to(s, 0, 2), to(s, 2, 2), send_p.at[s], recv_p.at[s], partner)

    def own(i):
        return held.at[0, :, at(i)]

    gain = gain_ref[...].astype(jnp.float32).reshape(1, cols)

    def norm(i):
        x_loads[i].wait()
        wide = x_s[i * piece : (i + 1) * piece, :].astype(jnp.float32)
        scale = lax.rsqrt(jnp.mean(wide * wide, -1, keepdims=True) + 1e-6)
        a = (wide * scale * gain).astype(jnp.bfloat16)
        for c in range(count):
            held[0, c, i * piece : (i + 1) * piece, :] = a[:, c * CHUNK : (c + 1) * CHUNK]

    norm(0)
    norm(2)
    to_right(own(0), 1).start()
    norm(1)
    to_left(own(2), 1).start()
    norm(3)
    for load in loads:
        load.start()
    to_right(own(1), 2).start()
    to_left(own(3), 2).start()
    to_partner(0).start()
    to_right(own(2), 3).start()
    to_left(own(0), 3).start()
    to_right(own(3), 4).start()
    to_left(own(1), 4).start()
    for load in loads:
        load.wait()

    first_half = lax.broadcasted_iota(jnp.int32, (1, HEAD), 1) < HEAD // 2
    outs = (k_s, v_s, q_s)
    all_heads, keys_values, queries = range(3 * heads), range(2 * heads), range(2 * heads, 3 * heads)

    def project(slot, low, size, starts, which):
        part = size // len(starts)
        turns = []
        for start in starts:
            j = start // piece
            near = pl.ds(pl.multiple_of(start - j * piece, part), part)
            c, s = far_ref[0, pl.ds(j, 1), :], far_ref[1, pl.ds(j, 1), :]
            cn, sn = near_ref[0, near, :], near_ref[1, near, :]
            turns.append((c * cn - s * sn, jnp.where(first_half, -1.0, 1.0) * (s * cn + c * sn)))
        cos = jnp.concatenate([t[0] for t in turns], axis=0)
        sin = jnp.concatenate([t[1] for t in turns], axis=0)
        for h0 in which[::4]:
            got = list(range(h0, min(h0 + 4, which[-1] + 1)))
            a = jnp.concatenate([held[slot, c, pl.ds(low, size), :] for c in range(count)], axis=1)
            t = _dot(a, w[:, h0 * HEAD : (got[-1] + 1) * HEAD], 1, 0).astype(jnp.bfloat16)
            for h in got:
                th = t[:, (h - h0) * HEAD : (h - h0 + 1) * HEAD]
                if h // heads != 1:
                    wide = th.astype(jnp.float32)
                    th = (wide * cos + pltpu.roll(wide, HEAD // 2, 1) * sin).astype(jnp.bfloat16)
                for i, start in enumerate(starts):
                    outs[h // heads][h % heads, pl.ds(pl.multiple_of(start, part), part), :] = th[i * part : (i + 1) * part, :]

    def step(i, _):
        slot, second = i // 2, i % 2
        t = slot - 1

        @pl.when(i == 2)
        def _():
            to_partner(0).wait_recv()

        @pl.when((i >= 4) & (second == 0))
        def _():
            to_right(own(0), t, long_lands).wait_recv()
            to_left(own(0), t, long_lands).wait_recv()
            to_partner(t, long_lands).start()

            @pl.when(t <= 2)
            def _():
                for r in range(2):
                    to_right(held.at[t + 1, :, pl.ds(r * short, short)], 2 * t + 3 + r).start()
                    to_left(held.at[t + 1, :, pl.ds(piece + r * short, short)], 2 * t + 3 + r).start()

        @pl.when((i >= 4) & (second == 1))
        def _():
            to_partner(t, long_lands).wait_recv()

        starts = []
        for r, (from_chip, part) in enumerate(((before, t - 1), (after, (t + 1) % 4))):
            landed_at = (2 * from_chip + jnp.where(second == 0, core, 1 - core)) * rows + part * piece
            whole_at = (2 * chip + jnp.where(i < 2, core, 1 - core)) * rows + (2 * second + r) * piece
            starts.append(jnp.where(i < 4, whole_at, landed_at))
        project(slot, pl.multiple_of(second * 2 * piece, 2 * piece), 2 * piece, starts, all_heads)
        return _

    def short_starts(s):
        return [(2 * across + (core if i < 2 else 1 - core)) * rows + ((s - 5) // 2 + 2 * (i % 2)) * piece + (s - 5) % 2 * short for i in range(4)]

    def hand_over(s):
        to_right(held.at[0, :, pl.ds(0, short)], s).wait_recv()
        to_left(held.at[0, :, pl.ds(0, short)], s).wait_recv()
        to_partner(s).start()


    hidden = lax.broadcasted_iota(jnp.int32, (rows, rows), 0) > lax.broadcasted_iota(jnp.int32, (rows, rows), 1)

    def block(u, to, keys, masked=False):
        here = pl.ds(pl.multiple_of(to * rows, rows), rows)
        keys = [pl.ds(pl.multiple_of(start, size), size) for start, size in keys]
        ones = jnp.ones((8, sum(k.size for k in keys)), jnp.bfloat16)

        def take(ref, h):
            parts = [ref[h, k, :] for k in keys]
            return parts[0] if len(parts) == 1 else jnp.concatenate(parts, axis=0)

        scores = [_dot(take(k_s, h), q_s[h, here, :], 1, 1) for h in range(heads)]
        weights, keeps = [], []
        for h, s in enumerate(scores):
            if masked:
                s = jnp.where(hidden, HIDDEN, s)
            old = top_s[u, h : h + 1, :]
            top = jnp.maximum(old, s.max(axis=0, keepdims=True))
            top_s[u, h : h + 1, :] = top
            weights.append(jnp.exp2((s - top) * e).astype(jnp.bfloat16))
            keeps.append(jnp.exp2((old - top) * e))
        for h, (p, keep) in enumerate(zip(weights, keeps)):
            values = jnp.concatenate([take(v_s, h).T, ones], axis=0)
            mix_s[u, h] = mix_s[u, h] * keep + _dot(values, p, 1, 0)

    def blocks(u, to, low, high):
        def run(j, _):
            block(u, to, [(j * rows, rows)])
            return _

        lax.fori_loop(low, high, run, None)

    def clear(u):
        top_s[u] = jnp.full(top_s.shape[1:], NEG, jnp.float32)
        mix_s[u] = jnp.zeros(mix_s.shape[1:], jnp.float32)

    def unit(u):
        to_chip = jnp.where(u < 2, after, before)
        return to_chip, 2 * to_chip + jnp.where(u % 2 == 0, 1 - core, core)

    def start_unit(u):
        to_chip, to = unit(u)
        clear(u)
        blocks(u, to, 0, jnp.minimum(2 * across, to))
        blocks(u, to, 2 * across + 2, to)
        block(u, to, [(to * rows, rows)], True)

    def finish(u, slot):
        for h in range(heads):
            o = mix_s[u, h, :HEAD, :] * (1 / mix_s[u, h, HEAD : HEAD + 1, :])
            seen[slot, :, h * HEAD : (h + 1) * HEAD] = o.T.astype(jnp.bfloat16)

    def go_on(u, s):
        to_chip, to = unit(u)

        @pl.when(across < to_chip)
        def _():
            block(u, to, [(start, short) for start in short_starts(s)])

    def attend(to, slot):
        clear(0)
        blocks(0, to, 0, to)
        block(0, to, [(to * rows, rows)], True)
        finish(0, slot)

    lax.fori_loop(0, 12, step, None)

    for u in range(1, 5):
        to_right(own(0), u).wait_send()
        to_left(own(0), u).wait_send()
    for u in range(5):
        to_partner(u).wait_send()
    for d in (left, right, partner):
        pl.semaphore_signal(ready1, inc=1, device_id={"tp": d}, device_id_type=MESH)

    def start_units(u, _):
        start_unit(u)

        @pl.when(u % 2 == 1)
        def _():
            hand_over(5 + u // 2)

        return _

    lax.fori_loop(0, 4, start_units, None)

    def short_step(s, _):
        to_partner(s).wait_recv()
        low = pl.multiple_of((s - 5) % 2 * 2 * piece, 2 * piece)
        project(6 + (s - 5) // 2, low, 2 * piece, short_starts(s), keys_values)

        @pl.when(s > 5)
        def _():
            hand_over(s + 1)

        lax.fori_loop(0, 4, lambda u, _: go_on(u, s), None)
        return _

    lax.fori_loop(5, 7, short_step, None)
    to_partner(7).wait_recv()
    project(7, 0, 2 * piece, short_starts(7), keys_values)
    lax.fori_loop(0, 4, lambda u, _: go_on(u, 7), None)
    hand_over(8)

    def last_half(i, _):
        @pl.when(i == 1)
        def _():
            to_partner(8).wait_recv()

        c = jnp.where(i == 0, core, 1 - core)
        starts = [(2 * across + c) * rows + (1 + 2 * r) * piece + short for r in range(2)]
        project(7, pl.multiple_of(2 * piece + i * piece, piece), piece, starts, keys_values)
        return _

    lax.fori_loop(0, 2, last_half, None)


    def columns(j):
        return pl.ds(pl.multiple_of(j * CHUNK, CHUNK), CHUNK)

    def spare(base, j):
        if base < 40:
            i = base + j
            return w.at[pl.ds(pl.multiple_of(i // 2 * rows, rows), rows), columns(i % 2)]
        return w.at[pl.ds(pl.multiple_of((base - 40 + j) * rows, rows), rows), columns(2)]

    right_at, left_at, y_at = (20, 30, 40), (25, 35, 45), 50

    def given(g, j):
        return spare(0, j % half) if g == 1 else spare(half, j % half) if g == 2 else spare(count, j)

    from_p_slots = (3, 0, 1, 6)

    def term(slot, j):
        return _dot(seen[slot], wo[:, columns(j)], 1, 0)

    def give_copy(g, j):
        return _send(given(g, j), held.at[from_p_slots[g], j], give_sem.at[g, j], give_got.at[g, j], partner)

    def ring_slot(base, part, j):
        return held.at[base, part * half + j] if part < 2 else held.at[2, (base - 4) * half + j]

    def right_copy(part, j):
        i = part * half + j
        return _send(spare(right_at[part], j), ring_slot(4, part, j), sum_r_sem.at[i], got_l.at[i], right)

    def left_copy(part, j):
        i = part * half + j
        return _send(spare(left_at[part], j), ring_slot(5, part, j), sum_l_sem.at[i], got_r.at[i], left)

    def landed_l(part, j):
        right_copy(part, j).wait_recv()
        return ring_slot(4, part, j)[...].astype(jnp.float32)

    def landed_r(part, j):
        left_copy(part, j).wait_recv()
        return ring_slot(5, part, j)[...].astype(jnp.float32)

    def give(*which):
        terms = [term(slot, j).astype(jnp.bfloat16) for g, slot, j, _ in which]
        for (g, slot, j, old), t in zip(which, terms):
            if old is not None:
                give_copy(*old).wait_send()
            given(g, j)[...] = t
        for g, slot, j, _ in which:
            give_copy(g, j).start()

    def pairs(*which):
        terms = [term(slot, j) for g, slot, j in which]
        for g, slot, j in which:
            give_copy(g, j).wait_recv()
        return [t + held[from_p_slots[g], j].astype(jnp.float32) for (g, slot, j), t in zip(which, terms)]

    def emit(part, j, rightwards, leftwards):
        spare(right_at[part], j)[...] = rightwards.astype(jnp.bfloat16)
        spare(left_at[part], j)[...] = leftwards.astype(jnp.bfloat16)
        right_copy(part, j).start()
        left_copy(part, j).start()

    def loop(body):
        def run(j, _):
            body(j)
            return _

        lax.fori_loop(0, half, run, None)

    def begin(j):
        give((1, 0, half + j, None), (2, 2, j, None))

    def part0(j):
        emit(0, j, *pairs((1, 1, half + j), (2, 3, j)))

        @pl.when(j < half - 1)
        def _():
            begin(j + 1)

    for u in (0, 2):
        go_on(u, 8)
        finish(u, u)
    pl.semaphore_wait(ready1, 3)
    begin(0)
    for u in (1, 3):
        go_on(u, 8)
        finish(u, u)
    for s in range(5, 9):
        to_right(held.at[0, :, pl.ds(0, short)], s).wait_send()
        to_left(held.at[0, :, pl.ds(0, short)], s).wait_send()
    for d in (left, right, partner):
        pl.semaphore_signal(ready2, inc=1, device_id={"tp": d}, device_id_type=MESH)
    loop(part0)

    project(6, 0, rows, short_starts(5) + short_starts(6), queries)
    project(7, 0, rows, short_starts(7) + short_starts(8), queries)
    for s in range(5, 9):
        to_partner(s).wait_send()
    pl.semaphore_signal(ready3, inc=1, device_id={"tp": partner}, device_id_type=MESH)
    attend(2 * across + 1 - core, 4)
    pl.semaphore_wait(ready2, 3)
    loop(lambda j: give((0, 4, j, None), (0, 4, half + j, None)))
    attend(2 * across + core, 4)
    loop(lambda j: emit(1, j, *pairs((0, 4, j), (0, 4, half + j))))

    loop(lambda j: give((1, 0, j, (1, half + j)), (2, 2, half + j, (2, j))))
    attend(2 * chip + 1 - core, 4)
    pl.semaphore_wait(ready3, 1)
    loop(lambda j: give((3, 4, j, (0, j)), (3, 4, half + j, (0, half + j))))
    attend(2 * chip + core, 4)

    def part2(j):
        a, b = pairs((1, 1, j), (2, 3, half + j))
        emit(2, j, a + landed_l(1, j), b + landed_r(1, j))

    loop(part2)

    def y_copy(j):
        return pltpu.make_async_copy(spare(y_at, j), y_hbm.at[:, columns(j)], y_sem.at[j])

    def last(j):
        a, b = pairs((3, 4, j), (3, 4, half + j))
        a += x_s[:, columns(j)].astype(jnp.float32)
        b += x_s[:, columns(half + j)].astype(jnp.float32)
        spare(y_at, j)[...] = (a + landed_r(0, j) + landed_l(2, j)).astype(jnp.bfloat16)
        y_copy(j).start()
        spare(y_at, half + j)[...] = (b + landed_l(0, j) + landed_r(2, j)).astype(jnp.bfloat16)
        y_copy(half + j).start()

    loop(last)

    def drain(j):
        for copy in (give_copy(1, j), give_copy(2, half + j), give_copy(3, j), give_copy(3, half + j)):
            copy.wait_send()
        for part in range(3):
            right_copy(part, j).wait_send()
            left_copy(part, j).wait_send()
        y_copy(j).wait()
        y_copy(half + j).wait()

    loop(drain)


def solution(mesh):
    n = mesh.shape["tp"]

    def step(x, gain, wq, wk, wv, wo):
        rows, cols = x.shape
        width = wq.shape[1]
        heads = width // HEAD
        tokens = n * rows
        count = cols // CHUNK
        ring = 3 * (count // 2)
        near, far = _tables(rows, rows // 4, tokens // (rows // 4))
        vmem, hbm = pl.BlockSpec(memory_space=pltpu.VMEM), pl.BlockSpec(memory_space=pl.ANY)
        dma = pltpu.SemaphoreType.DMA
        low = jnp.bfloat16
        return pl.pallas_call(
            functools.partial(layer, n),
            name="layer",
            out_shape=jax.ShapeDtypeStruct((rows, cols), low),
            in_specs=[hbm] + [vmem] * 3 + [hbm] * 4,
            out_specs=hbm,
            scratch_shapes=[
                pltpu.VMEM((rows, cols), low),
                pltpu.VMEM((8, count, rows, CHUNK), low),
                pltpu.VMEM((cols, 3 * width), low),
                pltpu.VMEM((width, cols), low),
                *[pltpu.VMEM((heads, tokens, HEAD), low)] * 3,
                pltpu.VMEM((5, rows, width), low),
                pltpu.VMEM((4, heads, rows), jnp.float32),
                pltpu.VMEM((4, heads, HEAD + 8, rows), jnp.float32),
                dma((4,)), dma((4,)), dma((8,)), dma((8,)), dma((9,)), dma((8,)), dma((8,)), dma((9,)),
                dma((4, count)), dma((4, count)), dma((ring,)), dma((ring,)), dma((ring,)), dma((ring,)), dma((count,)),
                *[pltpu.SemaphoreType.REGULAR] * 3,
            ],
            compiler_params=pltpu.CompilerParams(collective_id=0, has_side_effects=True, vmem_limit_bytes=VMEM),
        )(x, gain, jnp.asarray(near), jnp.asarray(far), wq, wk, wv, wo)

    tokens, columns = P(("dp", "tp"), None), P(None, "tp")
    return jax.shard_map(
        step,
        mesh=mesh,
        in_specs=(tokens, P(None), columns, columns, columns, P("tp", None)),
        out_specs=tokens,
        check_vma=False,
    )
```

```python
import functools

import jax
import jax.numpy as jnp
import numpy as np
from jax import lax
from jax.experimental import pallas as pl
from jax.experimental.pallas import tpu as pltpu
from jax.sharding import PartitionSpec as P

HEAD = 128
THETA = 10000
NEG = -1e30
HIDDEN = 2 * NEG
LOG2E = 1.4426950408889634
VMEM = 64_400_000
CHUNK = 512
MESH = pl.DeviceIdType.MESH


def _dot(a, b, ca, cb):
    return lax.dot_general(a, b, (((ca,), (cb,)), ((), ())), preferred_element_type=jnp.float32)


def _places(n):
    me = lax.axis_index("tp")
    chips = n // 2
    chip, core = me // 2, me % 2
    right = 2 * ((chip + 1) % chips) + core
    left = 2 * ((chip + chips - 1) % chips) + core
    return chip, core, left, right, 2 * chip + 1 - core


def _greet(devices):
    for d in devices:
        pl.semaphore_signal(pltpu.get_barrier_semaphore(), inc=1, device_id={"tp": d}, device_id_type=MESH)


def _send(src, dst, send_sem, recv_sem, device):
    return pltpu.make_async_remote_copy(src_ref=src, dst_ref=dst, send_sem=send_sem, recv_sem=recv_sem, device_id={"tp": device}, device_id_type=MESH)


def _tables(rows, piece, count):
    half = HEAD // 2
    step = float(THETA) ** (-np.arange(half, dtype=np.float64) / half)

    def pair(place):
        angle = place[:, None] * np.concatenate([step, step])[None, :]
        return np.stack([np.cos(angle), np.sin(angle)]).astype(np.float32)

    return pair(np.arange(piece, dtype=np.float64)), pair(piece * np.arange(count, dtype=np.float64))


def layer(n, x_hbm, gain_hbm, near_hbm, far_hbm, wq_hbm, wk_hbm, wv_hbm, wo_hbm, y_ref, gain_ref, near_ref, far_ref, held, w, wo, q_s, k_s, v_s, seen, top_s, mix_s,
          x_sem, w_sem, send_r, send_l, send_p, recv_r, recv_l, recv_p, give_sem, give_got, sum_r_sem, sum_l_sem, got_l, got_r, y_sem, ready1, ready2, ready3):
    chip, core, left, right, partner = _places(n)
    chips = n // 2
    rows, cols = x_hbm.shape
    heads = q_s.shape[0]
    width = heads * HEAD
    piece, short = rows // 4, rows // 8
    count = cols // CHUNK
    half = count // 2
    e = HEAD**-0.5 * LOG2E
    across, after, before = (chip + 2) % chips, (chip + 1) % chips, (chip + chips - 1) % chips

    x_loads = [pltpu.make_async_copy(x_hbm.at[pl.ds(i * piece, piece)], wo.at[pl.ds(i * piece, piece)], x_sem.at[i]) for i in range(4)]
    smalls = [pltpu.make_async_copy(src, dst, w_sem.at[4 + i]) for i, (src, dst) in enumerate(((gain_hbm, gain_ref), (near_hbm, near_ref), (far_hbm, far_ref)))]
    smalls[0].start()
    for load in x_loads:
        load.start()
    _greet((left, right, partner))
    loads = [pltpu.make_async_copy(src, w.at[:, pl.ds(i * width, width)], w_sem.at[i]) for i, src in enumerate((wk_hbm, wv_hbm, wq_hbm))]
    loads.append(pltpu.make_async_copy(wo_hbm, wo, w_sem.at[3]))


    def at(i):
        return pl.ds(i * piece, piece)

    def lands(s, quarter, quarters=1):
        if isinstance(s, int) and s < 5:
            return held.at[s + 1, :, pl.ds(quarter * piece, quarters * piece)]
        return held.at[6 + (s - 5) // 2, :, pl.ds(pl.multiple_of((s - 5) % 2 * 2 * piece + quarter * short, short), quarters * short)]

    def long_lands(s, quarter, quarters=1):
        return held.at[s + 1, :, pl.ds(quarter * piece, quarters * piece)]

    def to_right(src, s, to=lands):
        return _send(src, to(s, 0), send_r.at[s - 1], recv_l.at[s - 1], right)

    def to_left(src, s, to=lands):
        return _send(src, to(s, 1), send_l.at[s - 1], recv_r.at[s - 1], left)

    def to_partner(s, to=lands):
        if isinstance(s, int) and s == 0:
            return _send(held.at[0], held.at[1], send_p.at[0], recv_p.at[0], partner)
        return _send(to(s, 0, 2), to(s, 2, 2), send_p.at[s], recv_p.at[s], partner)

    def own(i):
        return held.at[0, :, at(i)]

    smalls[0].wait()
    gain = gain_ref[...].astype(jnp.float32).reshape(1, cols)

    def norm(i):
        x_loads[i].wait()
        wide = wo[i * piece : (i + 1) * piece, :].astype(jnp.float32)
        scale = lax.rsqrt(jnp.mean(wide * wide, -1, keepdims=True) + 1e-6)
        a = (wide * scale * gain).astype(jnp.bfloat16)
        for c in range(count):
            held[0, c, i * piece : (i + 1) * piece, :] = a[:, c * CHUNK : (c + 1) * CHUNK]

    norm(0)
    norm(2)
    pl.semaphore_wait(pltpu.get_barrier_semaphore(), 3)
    to_right(own(0), 1).start()
    norm(1)
    to_left(own(2), 1).start()
    norm(3)
    for load in smalls[1:] + loads:
        load.start()
    to_right(own(1), 2).start()
    to_left(own(3), 2).start()
    to_partner(0).start()
    to_right(own(2), 3).start()
    to_left(own(0), 3).start()
    to_right(own(3), 4).start()
    to_left(own(1), 4).start()
    for load in smalls[1:] + loads[:3]:
        load.wait()

    first_half = lax.broadcasted_iota(jnp.int32, (1, HEAD), 1) < HEAD // 2
    outs = (k_s, v_s, q_s)
    all_heads, keys_values, queries = range(3 * heads), range(2 * heads), range(2 * heads, 3 * heads)

    def project(slot, low, size, starts, which):
        part = size // len(starts)
        turns = []
        for start in starts:
            j = start // piece
            near = pl.ds(pl.multiple_of(start - j * piece, part), part)
            c, s = far_ref[0, pl.ds(j, 1), :], far_ref[1, pl.ds(j, 1), :]
            cn, sn = near_ref[0, near, :], near_ref[1, near, :]
            turns.append((c * cn - s * sn, jnp.where(first_half, -1.0, 1.0) * (s * cn + c * sn)))
        cos = jnp.concatenate([t[0] for t in turns], axis=0)
        sin = jnp.concatenate([t[1] for t in turns], axis=0)
        for h0 in which[::4]:
            got = list(range(h0, min(h0 + 4, which[-1] + 1)))
            a = jnp.concatenate([held[slot, c, pl.ds(low, size), :] for c in range(count)], axis=1)
            t = _dot(a, w[:, h0 * HEAD : (got[-1] + 1) * HEAD], 1, 0).astype(jnp.bfloat16)
            for h in got:
                th = t[:, (h - h0) * HEAD : (h - h0 + 1) * HEAD]
                if h // heads != 1:
                    wide = th.astype(jnp.float32)
                    th = (wide * cos + pltpu.roll(wide, HEAD // 2, 1) * sin).astype(jnp.bfloat16)
                for i, start in enumerate(starts):
                    outs[h // heads][h % heads, pl.ds(pl.multiple_of(start, part), part), :] = th[i * part : (i + 1) * part, :]

    def step(i, _):
        slot, second = i // 2, i % 2
        t = slot - 1

        @pl.when(i == 2)
        def _():
            to_partner(0).wait_recv()

        @pl.when((i >= 4) & (second == 0))
        def _():
            to_right(own(0), t, long_lands).wait_recv()
            to_left(own(0), t, long_lands).wait_recv()
            to_partner(t, long_lands).start()

            @pl.when(t <= 2)
            def _():
                for r in range(2):
                    to_right(held.at[t + 1, :, pl.ds(r * short, short)], 2 * t + 3 + r).start()
                    to_left(held.at[t + 1, :, pl.ds(piece + r * short, short)], 2 * t + 3 + r).start()

        @pl.when((i >= 4) & (second == 1))
        def _():
            to_partner(t, long_lands).wait_recv()

        starts = []
        for r, (from_chip, part) in enumerate(((before, t - 1), (after, (t + 1) % 4))):
            landed_at = (2 * from_chip + jnp.where(second == 0, core, 1 - core)) * rows + part * piece
            whole_at = (2 * chip + jnp.where(i < 2, core, 1 - core)) * rows + (2 * second + r) * piece
            starts.append(jnp.where(i < 4, whole_at, landed_at))
        project(slot, pl.multiple_of(second * 2 * piece, 2 * piece), 2 * piece, starts, all_heads)
        return _

    def short_starts(s):
        return [(2 * across + (core if i < 2 else 1 - core)) * rows + ((s - 5) // 2 + 2 * (i % 2)) * piece + (s - 5) % 2 * short for i in range(4)]

    def hand_over(s):
        to_right(held.at[0, :, pl.ds(0, short)], s).wait_recv()
        to_left(held.at[0, :, pl.ds(0, short)], s).wait_recv()
        to_partner(s).start()


    hidden = lax.broadcasted_iota(jnp.int32, (rows, rows), 0) > lax.broadcasted_iota(jnp.int32, (rows, rows), 1)

    def block(u, to, keys, masked=False):
        here = pl.ds(pl.multiple_of(to * rows, rows), rows)
        keys = [pl.ds(pl.multiple_of(start, size), size) for start, size in keys]
        ones = jnp.ones((8, sum(k.size for k in keys)), jnp.bfloat16)

        def take(ref, h):
            parts = [ref[h, k, :] for k in keys]
            return parts[0] if len(parts) == 1 else jnp.concatenate(parts, axis=0)

        scores = [_dot(take(k_s, h), q_s[h, here, :], 1, 1) for h in range(heads)]
        weights, keeps = [], []
        for h, s in enumerate(scores):
            if masked:
                s = jnp.where(hidden, HIDDEN, s)
            old = top_s[u, h : h + 1, :]
            top = jnp.maximum(old, s.max(axis=0, keepdims=True))
            top_s[u, h : h + 1, :] = top
            weights.append(jnp.exp2((s - top) * e).astype(jnp.bfloat16))
            keeps.append(jnp.exp2((old - top) * e))
        for h, (p, keep) in enumerate(zip(weights, keeps)):
            values = jnp.concatenate([take(v_s, h).T, ones], axis=0)
            mix_s[u, h] = mix_s[u, h] * keep + _dot(values, p, 1, 0)

    def blocks(u, to, low, high):
        def run(j, _):
            block(u, to, [(j * rows, rows)])
            return _

        lax.fori_loop(low, high, run, None)

    def clear(u):
        top_s[u] = jnp.full(top_s.shape[1:], NEG, jnp.float32)
        mix_s[u] = jnp.zeros(mix_s.shape[1:], jnp.float32)

    def unit(u):
        to_chip = jnp.where(u < 2, after, before)
        return to_chip, 2 * to_chip + jnp.where(u % 2 == 0, 1 - core, core)

    def start_unit(u):
        to_chip, to = unit(u)
        clear(u)
        blocks(u, to, 0, jnp.minimum(2 * across, to))
        blocks(u, to, 2 * across + 2, to)
        block(u, to, [(to * rows, rows)], True)

    def finish(u, slot):
        for h in range(heads):
            o = mix_s[u, h, :HEAD, :] * (1 / mix_s[u, h, HEAD : HEAD + 1, :])
            seen[slot, :, h * HEAD : (h + 1) * HEAD] = o.T.astype(jnp.bfloat16)

    def go_on(u, s):
        to_chip, to = unit(u)

        @pl.when(across < to_chip)
        def _():
            block(u, to, [(start, short) for start in short_starts(s)])

    def attend(to, slot):
        clear(0)
        blocks(0, to, 0, to)
        block(0, to, [(to * rows, rows)], True)
        finish(0, slot)

    lax.fori_loop(0, 12, step, None)

    for u in range(1, 5):
        to_right(own(0), u).wait_send()
        to_left(own(0), u).wait_send()
    for u in range(5):
        to_partner(u).wait_send()
    for d in (left, right, partner):
        pl.semaphore_signal(ready1, inc=1, device_id={"tp": d}, device_id_type=MESH)

    def start_units(u, _):
        start_unit(u)

        @pl.when(u % 2 == 1)
        def _():
            hand_over(5 + u // 2)

        return _

    lax.fori_loop(0, 4, start_units, None)

    def short_step(s, _):
        to_partner(s).wait_recv()
        low = pl.multiple_of((s - 5) % 2 * 2 * piece, 2 * piece)
        project(6 + (s - 5) // 2, low, 2 * piece, short_starts(s), keys_values)

        @pl.when(s > 5)
        def _():
            hand_over(s + 1)

        lax.fori_loop(0, 4, lambda u, _: go_on(u, s), None)
        return _

    lax.fori_loop(5, 7, short_step, None)
    to_partner(7).wait_recv()
    project(7, 0, 2 * piece, short_starts(7), keys_values)
    lax.fori_loop(0, 4, lambda u, _: go_on(u, 7), None)
    hand_over(8)

    project(6, 0, rows, short_starts(5) + short_starts(6), queries)
    to_partner(8).wait_recv()
    project(7, 2 * piece, 2 * piece, short_starts(8), keys_values)


    def columns(j):
        return pl.ds(pl.multiple_of(j * CHUNK, CHUNK), CHUNK)

    def spare(base, j):
        if base < 40:
            i = base + j
            return w.at[pl.ds(pl.multiple_of(i // 2 * rows, rows), rows), columns(i % 2)]
        return w.at[pl.ds(pl.multiple_of((base - 40 + j) * rows, rows), rows), columns(2)]

    right_at, left_at, y_at = (20, 30, 40), (25, 35, 45), 50

    def given(g, j):
        return spare(0, j % half) if g == 1 else spare(half, j % half) if g == 2 else spare(count, j)

    from_p_slots = (3, 0, 1, 6)

    def term(slot, j):
        return _dot(seen[slot], wo[:, columns(j)], 1, 0)

    def give_copy(g, j):
        return _send(given(g, j), held.at[from_p_slots[g], j], give_sem.at[g, j], give_got.at[g, j], partner)

    def ring_slot(base, part, j):
        return held.at[base, part * half + j] if part < 2 else held.at[2, (base - 4) * half + j]

    def right_copy(part, j):
        i = part * half + j
        return _send(spare(right_at[part], j), ring_slot(4, part, j), sum_r_sem.at[i], got_l.at[i], right)

    def left_copy(part, j):
        i = part * half + j
        return _send(spare(left_at[part], j), ring_slot(5, part, j), sum_l_sem.at[i], got_r.at[i], left)

    def landed_l(part, j):
        right_copy(part, j).wait_recv()
        return ring_slot(4, part, j)[...].astype(jnp.float32)

    def landed_r(part, j):
        left_copy(part, j).wait_recv()
        return ring_slot(5, part, j)[...].astype(jnp.float32)

    def give(*which):
        terms = [term(slot, j).astype(jnp.bfloat16) for g, slot, j, _ in which]
        for (g, slot, j, old), t in zip(which, terms):
            if old is not None:
                give_copy(*old).wait_send()
            given(g, j)[...] = t
        for g, slot, j, _ in which:
            give_copy(g, j).start()

    def pairs(*which):
        terms = [term(slot, j) for g, slot, j in which]
        for g, slot, j in which:
            give_copy(g, j).wait_recv()
        return [t + held[from_p_slots[g], j].astype(jnp.float32) for (g, slot, j), t in zip(which, terms)]

    def emit(part, j, rightwards, leftwards):
        spare(right_at[part], j)[...] = rightwards.astype(jnp.bfloat16)
        spare(left_at[part], j)[...] = leftwards.astype(jnp.bfloat16)
        right_copy(part, j).start()
        left_copy(part, j).start()

    def loop(body):
        def run(j, _):
            body(j)
            return _

        lax.fori_loop(0, half, run, None)

    x_again = [pltpu.make_async_copy(x_hbm.at[:, columns(j)], held.at[7, j], x_sem.at[4 + j]) for j in range(count)]

    def begin(j):
        give((1, 0, half + j, None), (2, 2, j, None))

    def part0(j):
        emit(0, j, *pairs((1, 1, half + j), (2, 3, j)))

        @pl.when(j < half - 1)
        def _():
            begin(j + 1)

    for u in (0, 2):
        go_on(u, 8)
        finish(u, u)
    loads[3].wait()
    pl.semaphore_wait(ready1, 3)
    begin(0)
    for u in (1, 3):
        go_on(u, 8)
        finish(u, u)
    for s in range(5, 9):
        to_right(held.at[0, :, pl.ds(0, short)], s).wait_send()
        to_left(held.at[0, :, pl.ds(0, short)], s).wait_send()
    for d in (left, right, partner):
        pl.semaphore_signal(ready2, inc=1, device_id={"tp": d}, device_id_type=MESH)
    loop(part0)

    project(7, 0, rows, short_starts(7) + short_starts(8), queries)
    for s in range(5, 9):
        to_partner(s).wait_send()
    pl.semaphore_signal(ready3, inc=1, device_id={"tp": partner}, device_id_type=MESH)
    for load in x_again:
        load.start()
    attend(2 * across + 1 - core, 4)
    pl.semaphore_wait(ready2, 3)
    loop(lambda j: give((0, 4, j, None), (0, 4, half + j, None)))
    attend(2 * across + core, 4)
    loop(lambda j: emit(1, j, *pairs((0, 4, j), (0, 4, half + j))))

    loop(lambda j: give((1, 0, j, (1, half + j)), (2, 2, half + j, (2, j))))
    attend(2 * chip + 1 - core, 4)
    pl.semaphore_wait(ready3, 1)
    loop(lambda j: give((3, 4, j, (0, j)), (3, 4, half + j, (0, half + j))))
    attend(2 * chip + core, 4)

    def part2(j):
        a, b = pairs((1, 1, j), (2, 3, half + j))
        emit(2, j, a + landed_l(1, j), b + landed_r(1, j))

    loop(part2)

    def y_copy(j):
        return pltpu.make_async_copy(spare(y_at, j), y_ref.at[:, columns(j)], y_sem.at[j])

    def last(j):
        a, b = pairs((3, 4, j), (3, 4, half + j))
        a += held[7, j].astype(jnp.float32)
        b += held[7, half + j].astype(jnp.float32)
        spare(y_at, j)[...] = (a + landed_r(0, j) + landed_l(2, j)).astype(jnp.bfloat16)
        y_copy(j).start()
        spare(y_at, half + j)[...] = (b + landed_l(0, j) + landed_r(2, j)).astype(jnp.bfloat16)
        y_copy(half + j).start()

    for load in x_again:
        load.wait()
    loop(last)

    def drain(j):
        for copy in (give_copy(1, j), give_copy(2, half + j), give_copy(3, j), give_copy(3, half + j)):
            copy.wait_send()
        for part in range(3):
            right_copy(part, j).wait_send()
            left_copy(part, j).wait_send()
        y_copy(j).wait()
        y_copy(half + j).wait()

    loop(drain)


def solution(mesh):
    n = mesh.shape["tp"]

    def step(x, gain, wq, wk, wv, wo):
        rows, cols = x.shape
        width = wq.shape[1]
        heads = width // HEAD
        tokens = n * rows
        count = cols // CHUNK
        ring = 3 * (count // 2)
        near, far = _tables(rows, rows // 4, tokens // (rows // 4))
        hbm = pl.BlockSpec(memory_space=pl.ANY)
        dma = pltpu.SemaphoreType.DMA
        low = jnp.bfloat16
        return pl.pallas_call(
            functools.partial(layer, n),
            name="layer",
            out_shape=pltpu.VMEM((rows, cols), low),
            in_specs=[hbm] * 8,
            out_specs=hbm,
            scratch_shapes=[
                pltpu.VMEM((cols,), low),
                pltpu.VMEM(near.shape, jnp.float32),
                pltpu.VMEM(far.shape, jnp.float32),
                pltpu.VMEM((8, count, rows, CHUNK), low),
                pltpu.VMEM((cols, 3 * width), low),
                pltpu.VMEM((width, cols), low),
                *[pltpu.VMEM((heads, tokens, HEAD), low)] * 3,
                pltpu.VMEM((5, rows, width), low),
                pltpu.VMEM((4, heads, rows), jnp.float32),
                pltpu.VMEM((4, heads, HEAD + 8, rows), jnp.float32),
                dma((4 + count,)), dma((7,)), dma((8,)), dma((8,)), dma((9,)), dma((8,)), dma((8,)), dma((9,)),
                dma((4, count)), dma((4, count)), dma((ring,)), dma((ring,)), dma((ring,)), dma((ring,)), dma((count,)),
                *[pltpu.SemaphoreType.REGULAR] * 3,
            ],
            compiler_params=pltpu.CompilerParams(collective_id=0, has_side_effects=True, vmem_limit_bytes=VMEM),
        )(x, gain, jnp.asarray(near), jnp.asarray(far), wq, wk, wv, wo)

    tokens, columns = P(("dp", "tp"), None), P(None, "tp")
    return jax.shard_map(
        step,
        mesh=mesh,
        in_specs=(tokens, P(None), columns, columns, columns, P("tp", None)),
        out_specs=tokens,
        check_vma=False,
    )
```

```python
import functools

import jax
import jax.numpy as jnp
import numpy as np
from jax import lax
from jax.experimental import pallas as pl
from jax.experimental.pallas import tpu as pltpu
from jax.sharding import PartitionSpec as P

HEAD = 128
THETA = 10000
NEG = -1e30
HIDDEN = 2 * NEG
LOG2E = 1.4426950408889634
VMEM = 64_400_000
CHUNK = 512
MESH = pl.DeviceIdType.MESH


def _dot(a, b, ca, cb):
    return lax.dot_general(a, b, (((ca,), (cb,)), ((), ())), preferred_element_type=jnp.float32)


def _places(n):
    me = lax.axis_index("tp")
    chips = n // 2
    chip, core = me // 2, me % 2
    right = 2 * ((chip + 1) % chips) + core
    left = 2 * ((chip + chips - 1) % chips) + core
    return chip, core, left, right, 2 * chip + 1 - core


def _greet(devices):
    for d in devices:
        pl.semaphore_signal(pltpu.get_barrier_semaphore(), inc=1, device_id={"tp": d}, device_id_type=MESH)


def _send(src, dst, send_sem, recv_sem, device):
    return pltpu.make_async_remote_copy(src_ref=src, dst_ref=dst, send_sem=send_sem, recv_sem=recv_sem, device_id={"tp": device}, device_id_type=MESH)


def _tables(rows, piece, count):
    half = HEAD // 2
    step = float(THETA) ** (-np.arange(half, dtype=np.float64) / half)

    def pair(place):
        angle = place[:, None] * np.concatenate([step, step])[None, :]
        return np.stack([np.cos(angle), np.sin(angle)]).astype(np.float32)

    return pair(np.arange(piece, dtype=np.float64)), pair(piece * np.arange(count, dtype=np.float64))


def layer(n, x_hbm, gain_hbm, near_hbm, far_hbm, wq_hbm, wk_hbm, wv_hbm, wo_hbm, y_ref, gain_ref, near_ref, far_ref, held, w, wo, q_s, k_s, v_s, seen, top_s, mix_s,
          x_sem, w_sem, send_r, send_l, send_p, recv_r, recv_l, recv_p, give_sem, give_got, sum_r_sem, sum_l_sem, got_l, got_r, y_sem, ready1, ready2, ready3):
    chip, core, left, right, partner = _places(n)
    chips = n // 2
    rows, cols = x_hbm.shape
    heads = q_s.shape[0]
    width = heads * HEAD
    piece, short = rows // 4, rows // 8
    count = cols // CHUNK
    half = count // 2
    e = HEAD**-0.5 * LOG2E
    across, after, before = (chip + 2) % chips, (chip + 1) % chips, (chip + chips - 1) % chips

    x_loads = [pltpu.make_async_copy(x_hbm.at[pl.ds(i * piece, piece)], wo.at[pl.ds(i * piece, piece)], x_sem.at[i]) for i in range(4)]
    smalls = [pltpu.make_async_copy(src, dst, w_sem.at[4 + i]) for i, (src, dst) in enumerate(((gain_hbm, gain_ref), (near_hbm, near_ref), (far_hbm, far_ref)))]
    smalls[0].start()
    for i in (0, 2, 1, 3):
        x_loads[i].start()
    _greet((left, right, partner))
    loads = [pltpu.make_async_copy(src, w.at[:, pl.ds(i * width, width)], w_sem.at[i]) for i, src in enumerate((wk_hbm, wv_hbm, wq_hbm))]
    loads.append(pltpu.make_async_copy(wo_hbm, wo, w_sem.at[3]))


    def at(i):
        return pl.ds(i * piece, piece)

    def lands(s, quarter, quarters=1):
        if isinstance(s, int) and s < 5:
            return held.at[s + 1, :, pl.ds(quarter * piece, quarters * piece)]
        return held.at[6 + (s - 5) // 2, :, pl.ds(pl.multiple_of((s - 5) % 2 * 2 * piece + quarter * short, short), quarters * short)]

    def long_lands(s, quarter, quarters=1):
        return held.at[s + 1, :, pl.ds(quarter * piece, quarters * piece)]

    def to_right(src, s, to=lands):
        return _send(src, to(s, 0), send_r.at[s - 1], recv_l.at[s - 1], right)

    def to_left(src, s, to=lands):
        return _send(src, to(s, 1), send_l.at[s - 1], recv_r.at[s - 1], left)

    def to_partner(s, to=lands):
        if isinstance(s, int) and s == 0:
            return _send(held.at[0], held.at[1], send_p.at[0], recv_p.at[0], partner)
        return _send(to(s, 0, 2), to(s, 2, 2), send_p.at[s], recv_p.at[s], partner)

    def own(i):
        return held.at[0, :, at(i)]

    smalls[0].wait()
    gain = gain_ref[...].astype(jnp.float32).reshape(1, cols)

    def norm(i):
        x_loads[i].wait()
        wide = wo[i * piece : (i + 1) * piece, :].astype(jnp.float32)
        scale = lax.rsqrt(jnp.mean(wide * wide, -1, keepdims=True) + 1e-6)
        a = (wide * scale * gain).astype(jnp.bfloat16)
        for c in range(count):
            held[0, c, i * piece : (i + 1) * piece, :] = a[:, c * CHUNK : (c + 1) * CHUNK]

    norm(0)
    norm(2)
    pl.semaphore_wait(pltpu.get_barrier_semaphore(), 3)
    to_right(own(0), 1).start()
    norm(1)
    to_left(own(2), 1).start()
    norm(3)
    for load in smalls[1:] + loads:
        load.start()
    to_right(own(1), 2).start()
    to_left(own(3), 2).start()
    to_partner(0).start()
    to_right(own(2), 3).start()
    to_left(own(0), 3).start()
    to_right(own(3), 4).start()
    to_left(own(1), 4).start()
    for load in smalls[1:] + loads[:3]:
        load.wait()

    first_half = lax.broadcasted_iota(jnp.int32, (1, HEAD), 1) < HEAD // 2
    outs = (k_s, v_s, q_s)
    all_heads, keys_values, queries = range(3 * heads), range(2 * heads), range(2 * heads, 3 * heads)

    def project(slot, low, size, starts, which):
        part = size // len(starts)
        turns = []
        for start in starts:
            j = start // piece
            near = pl.ds(pl.multiple_of(start - j * piece, part), part)
            c, s = far_ref[0, pl.ds(j, 1), :], far_ref[1, pl.ds(j, 1), :]
            cn, sn = near_ref[0, near, :], near_ref[1, near, :]
            turns.append((c * cn - s * sn, jnp.where(first_half, -1.0, 1.0) * (s * cn + c * sn)))
        cos = jnp.concatenate([t[0] for t in turns], axis=0)
        sin = jnp.concatenate([t[1] for t in turns], axis=0)
        for h0 in which[::4]:
            got = list(range(h0, min(h0 + 4, which[-1] + 1)))
            a = jnp.concatenate([held[slot, c, pl.ds(low, size), :] for c in range(count)], axis=1)
            t = _dot(a, w[:, h0 * HEAD : (got[-1] + 1) * HEAD], 1, 0).astype(jnp.bfloat16)
            for h in got:
                th = t[:, (h - h0) * HEAD : (h - h0 + 1) * HEAD]
                if h // heads != 1:
                    wide = th.astype(jnp.float32)
                    th = (wide * cos + pltpu.roll(wide, HEAD // 2, 1) * sin).astype(jnp.bfloat16)
                for i, start in enumerate(starts):
                    outs[h // heads][h % heads, pl.ds(pl.multiple_of(start, part), part), :] = th[i * part : (i + 1) * part, :]

    def step(i, _):
        slot, second = i // 2, i % 2
        t = slot - 1

        @pl.when(i == 2)
        def _():
            to_partner(0).wait_recv()

        @pl.when((i >= 4) & (second == 0))
        def _():
            to_right(own(0), t, long_lands).wait_recv()
            to_left(own(0), t, long_lands).wait_recv()
            to_partner(t, long_lands).start()

            @pl.when(t <= 2)
            def _():
                for r in range(2):
                    to_right(held.at[t + 1, :, pl.ds(r * short, short)], 2 * t + 3 + r).start()
                    to_left(held.at[t + 1, :, pl.ds(piece + r * short, short)], 2 * t + 3 + r).start()

        @pl.when((i >= 4) & (second == 1))
        def _():
            to_partner(t, long_lands).wait_recv()

        starts = []
        for r, (from_chip, part) in enumerate(((before, t - 1), (after, (t + 1) % 4))):
            landed_at = (2 * from_chip + jnp.where(second == 0, core, 1 - core)) * rows + part * piece
            whole_at = (2 * chip + jnp.where(i < 2, core, 1 - core)) * rows + (2 * second + r) * piece
            starts.append(jnp.where(i < 4, whole_at, landed_at))
        project(slot, pl.multiple_of(second * 2 * piece, 2 * piece), 2 * piece, starts, all_heads)
        return _

    def short_starts(s):
        return [(2 * across + (core if i < 2 else 1 - core)) * rows + ((s - 5) // 2 + 2 * (i % 2)) * piece + (s - 5) % 2 * short for i in range(4)]

    def hand_over(s):
        to_right(held.at[0, :, pl.ds(0, short)], s).wait_recv()
        to_left(held.at[0, :, pl.ds(0, short)], s).wait_recv()
        to_partner(s).start()


    visible = lax.broadcasted_iota(jnp.int32, (rows, rows), 0) <= lax.broadcasted_iota(jnp.int32, (rows, rows), 1)

    def block(units, keys, sees):
        here = [pl.ds(pl.multiple_of(to * rows, rows), rows) for _, to in units]
        keys = [pl.ds(pl.multiple_of(start, size), size) for start, size in keys]
        ones = jnp.ones((8, sum(k.size for k in keys)), jnp.bfloat16)

        def joined(parts, axis):
            return parts[0] if len(parts) == 1 else jnp.concatenate(parts, axis=axis)

        def take(ref, h, where):
            return joined([ref[h, k, :] for k in where], 0)

        scores = [_dot(take(k_s, h, keys), take(q_s, h, here), 1, 1) for h in range(heads)]
        weights, keeps = [], []
        for h, s in enumerate(scores):
            if sees is not None:
                s = jnp.where(sees, s, HIDDEN)
            old = joined([top_s[u, h : h + 1, :] for u, _ in units], 1)
            top = jnp.maximum(old, s.max(axis=0, keepdims=True))
            for i, (u, _) in enumerate(units):
                top_s[u, h : h + 1, :] = top[:, i * rows : (i + 1) * rows]
            weights.append(jnp.exp2((s - top) * e).astype(jnp.bfloat16))
            keeps.append(jnp.exp2((old - top) * e))
        for h, (p, keep) in enumerate(zip(weights, keeps)):
            mixed = _dot(jnp.concatenate([take(v_s, h, keys).T, ones], axis=0), p, 1, 0)
            for i, (u, _) in enumerate(units):
                part = slice(i * rows, (i + 1) * rows)
                mix_s[u, h] = mix_s[u, h] * keep[:, part] + mixed[:, part]

    def blocks(u, to, low, high):
        def run(j, _):
            block([(u, to)], [(j * rows, rows)], None)
            return _

        lax.fori_loop(low, high, run, None)

    def clear(u):
        top_s[u] = jnp.full(top_s.shape[1:], NEG, jnp.float32)
        mix_s[u] = jnp.zeros(mix_s.shape[1:], jnp.float32)

    def unit(u):
        to_chip = jnp.where(u < 2, after, before)
        return to_chip, 2 * to_chip + jnp.where(u % 2 == 0, 1 - core, core)

    def start_unit(u):
        to_chip, to = unit(u)
        clear(u)
        blocks(u, to, 0, jnp.minimum(2 * across, to))
        blocks(u, to, 2 * across + 2, to)
        block([(u, to)], [(to * rows, rows)], visible)

    def finish(u, slot):
        for h in range(heads):
            o = mix_s[u, h, :HEAD, :] * (1 / mix_s[u, h, HEAD : HEAD + 1, :])
            seen[slot, :, h * HEAD : (h + 1) * HEAD] = o.T.astype(jnp.bfloat16)

    def go_on(u, s):
        (to_chip, a), (_, b) = unit(u), unit(u + 1)

        @pl.when(across < to_chip)
        def _():
            block([(u, a), (u + 1, b)], [(start, short) for start in short_starts(s)], None)

    def attend(to, slot):
        clear(0)
        blocks(0, to, 0, to)
        block([(0, to)], [(to * rows, rows)], visible)
        finish(0, slot)

    lax.fori_loop(0, 12, step, None)

    for u in range(1, 5):
        to_right(own(0), u).wait_send()
        to_left(own(0), u).wait_send()
    for u in range(5):
        to_partner(u).wait_send()
    for d in (left, right, partner):
        pl.semaphore_signal(ready1, inc=1, device_id={"tp": d}, device_id_type=MESH)

    def start_units(u, _):
        start_unit(u)

        @pl.when(u % 2 == 1)
        def _():
            hand_over(5 + u // 2)

        return _

    lax.fori_loop(0, 4, start_units, None)

    def short_step(s, _):
        to_partner(s).wait_recv()
        low = pl.multiple_of((s - 5) % 2 * 2 * piece, 2 * piece)
        project(6 + (s - 5) // 2, low, 2 * piece, short_starts(s), keys_values)

        @pl.when(s > 5)
        def _():
            hand_over(s + 1)

        lax.fori_loop(0, 2, lambda i, _: go_on(2 * i, s), None)
        return _

    lax.fori_loop(5, 7, short_step, None)
    to_partner(7).wait_recv()
    project(7, 0, 2 * piece, short_starts(7), keys_values)
    lax.fori_loop(0, 2, lambda i, _: go_on(2 * i, 7), None)

    idle = (after < across) & (before < across)

    @pl.when(idle)
    def _():
        project(6, 0, rows, short_starts(5) + short_starts(6), queries)

    hand_over(8)

    @pl.when(jnp.logical_not(idle))
    def _():
        project(6, 0, 2 * piece, short_starts(5), queries)

    to_partner(8).wait_recv()
    project(7, 2 * piece, 2 * piece, short_starts(8), keys_values)


    def columns(j):
        return pl.ds(pl.multiple_of(j * CHUNK, CHUNK), CHUNK)

    def spare(base, j):
        if base < 40:
            i = base + j
            return w.at[pl.ds(pl.multiple_of(i // 2 * rows, rows), rows), columns(i % 2)]
        return w.at[pl.ds(pl.multiple_of((base - 40 + j) * rows, rows), rows), columns(2)]

    right_at, left_at, y_at = (20, 30, 40), (25, 35, 45), 50

    def given(g, j):
        return spare(0, j % half) if g == 1 else spare(half, j % half) if g == 2 else spare(count, j)

    from_p_slots = (3, 0, 1, 6)

    def term(slot, j):
        return _dot(seen[slot], wo[:, columns(j)], 1, 0)

    def give_copy(g, j):
        return _send(given(g, j), held.at[from_p_slots[g], j], give_sem.at[g, j], give_got.at[g, j], partner)

    def ring_slot(base, part, j):
        return held.at[base, part * half + j] if part < 2 else held.at[2, (base - 4) * half + j]

    def right_copy(part, j):
        i = part * half + j
        return _send(spare(right_at[part], j), ring_slot(4, part, j), sum_r_sem.at[i], got_l.at[i], right)

    def left_copy(part, j):
        i = part * half + j
        return _send(spare(left_at[part], j), ring_slot(5, part, j), sum_l_sem.at[i], got_r.at[i], left)

    def landed_l(part, j):
        right_copy(part, j).wait_recv()
        return ring_slot(4, part, j)[...].astype(jnp.float32)

    def landed_r(part, j):
        left_copy(part, j).wait_recv()
        return ring_slot(5, part, j)[...].astype(jnp.float32)

    def give(*which):
        terms = [term(slot, j).astype(jnp.bfloat16) for g, slot, j, _ in which]
        for (g, slot, j, old), t in zip(which, terms):
            if old is not None:
                give_copy(*old).wait_send()
            given(g, j)[...] = t
        for g, slot, j, _ in which:
            give_copy(g, j).start()

    def pairs(*which):
        terms = [term(slot, j) for g, slot, j in which]
        for g, slot, j in which:
            give_copy(g, j).wait_recv()
        return [t + held[from_p_slots[g], j].astype(jnp.float32) for (g, slot, j), t in zip(which, terms)]

    def emit(part, j, rightwards, leftwards):
        spare(right_at[part], j)[...] = rightwards.astype(jnp.bfloat16)
        spare(left_at[part], j)[...] = leftwards.astype(jnp.bfloat16)
        right_copy(part, j).start()
        left_copy(part, j).start()

    def loop(body):
        def run(j, _):
            body(j)
            return _

        lax.fori_loop(0, half, run, None)

    x_again = [pltpu.make_async_copy(x_hbm.at[:, columns(j)], held.at[7, j], x_sem.at[4 + j]) for j in range(count)]

    def begin(j):
        give((1, 0, half + j, None), (2, 2, j, None))

    def part0(j):
        emit(0, j, *pairs((1, 1, half + j), (2, 3, j)))

        @pl.when(j < half - 1)
        def _():
            begin(j + 1)

    go_on(0, 8)
    go_on(2, 8)
    finish(0, 0)
    finish(2, 2)
    loads[3].wait()
    pl.semaphore_wait(ready1, 3)
    begin(0)
    finish(1, 1)
    finish(3, 3)
    for s in range(5, 9):
        to_right(held.at[0, :, pl.ds(0, short)], s).wait_send()
        to_left(held.at[0, :, pl.ds(0, short)], s).wait_send()
    for d in (left, right, partner):
        pl.semaphore_signal(ready2, inc=1, device_id={"tp": d}, device_id_type=MESH)
    loop(part0)

    @pl.when(jnp.logical_not(idle))
    def _():
        project(6, 2 * piece, 2 * piece, short_starts(6), queries)

    project(7, 0, rows, short_starts(7) + short_starts(8), queries)
    for s in range(5, 9):
        to_partner(s).wait_send()
    pl.semaphore_signal(ready3, inc=1, device_id={"tp": partner}, device_id_type=MESH)
    for load in x_again:
        load.start()
    attend(2 * across + 1 - core, 4)
    pl.semaphore_wait(ready2, 3)
    loop(lambda j: give((0, 4, j, None), (0, 4, half + j, None)))
    attend(2 * across + core, 4)
    loop(lambda j: emit(1, j, *pairs((0, 4, j), (0, 4, half + j))))

    loop(lambda j: give((1, 0, j, (1, half + j)), (2, 2, half + j, (2, j))))
    attend(2 * chip + 1 - core, 4)
    pl.semaphore_wait(ready3, 1)
    loop(lambda j: give((3, 4, j, (0, j)), (3, 4, half + j, (0, half + j))))
    attend(2 * chip + core, 4)

    def part2(j):
        a, b = pairs((1, 1, j), (2, 3, half + j))
        emit(2, j, a + landed_l(1, j), b + landed_r(1, j))

    loop(part2)

    def y_copy(j):
        return pltpu.make_async_copy(spare(y_at, j), y_ref.at[:, columns(j)], y_sem.at[j])

    def last(j):
        a, b = pairs((3, 4, j), (3, 4, half + j))
        a += held[7, j].astype(jnp.float32)
        b += held[7, half + j].astype(jnp.float32)
        spare(y_at, j)[...] = (a + landed_r(0, j) + landed_l(2, j)).astype(jnp.bfloat16)
        y_copy(j).start()
        spare(y_at, half + j)[...] = (b + landed_l(0, j) + landed_r(2, j)).astype(jnp.bfloat16)
        y_copy(half + j).start()

    for load in x_again:
        load.wait()
    loop(last)

    def drain(j):
        for copy in (give_copy(1, j), give_copy(2, half + j), give_copy(3, j), give_copy(3, half + j)):
            copy.wait_send()
        for part in range(3):
            right_copy(part, j).wait_send()
            left_copy(part, j).wait_send()
        y_copy(j).wait()
        y_copy(half + j).wait()

    loop(drain)


def solution(mesh):
    n = mesh.shape["tp"]

    def step(x, gain, wq, wk, wv, wo):
        rows, cols = x.shape
        width = wq.shape[1]
        heads = width // HEAD
        tokens = n * rows
        count = cols // CHUNK
        ring = 3 * (count // 2)
        near, far = _tables(rows, rows // 4, tokens // (rows // 4))
        hbm = pl.BlockSpec(memory_space=pl.ANY)
        dma = pltpu.SemaphoreType.DMA
        low = jnp.bfloat16
        return pl.pallas_call(
            functools.partial(layer, n),
            name="layer",
            out_shape=pltpu.VMEM((rows, cols), low),
            in_specs=[hbm] * 8,
            out_specs=hbm,
            scratch_shapes=[
                pltpu.VMEM((cols,), low),
                pltpu.VMEM(near.shape, jnp.float32),
                pltpu.VMEM(far.shape, jnp.float32),
                pltpu.VMEM((8, count, rows, CHUNK), low),
                pltpu.VMEM((cols, 3 * width), low),
                pltpu.VMEM((width, cols), low),
                *[pltpu.VMEM((heads, tokens, HEAD), low)] * 3,
                pltpu.VMEM((5, rows, width), low),
                pltpu.VMEM((4, heads, rows), jnp.float32),
                pltpu.VMEM((4, heads, HEAD + 8, rows), jnp.float32),
                dma((4 + count,)), dma((7,)), dma((8,)), dma((8,)), dma((9,)), dma((8,)), dma((8,)), dma((9,)),
                dma((4, count)), dma((4, count)), dma((ring,)), dma((ring,)), dma((ring,)), dma((ring,)), dma((count,)),
                *[pltpu.SemaphoreType.REGULAR] * 3,
            ],
            compiler_params=pltpu.CompilerParams(collective_id=0, has_side_effects=True, vmem_limit_bytes=VMEM),
        )(x, gain, jnp.asarray(near), jnp.asarray(far), wq, wk, wv, wo)

    tokens, columns = P(("dp", "tp"), None), P(None, "tp")
    return jax.shard_map(
        step,
        mesh=mesh,
        in_specs=(tokens, P(None), columns, columns, columns, P("tp", None)),
        out_specs=tokens,
        check_vma=False,
    )
```

```python
import functools

import jax
import jax.numpy as jnp
import numpy as np
from jax import lax
from jax.experimental import pallas as pl
from jax.experimental.pallas import tpu as pltpu
from jax.sharding import PartitionSpec as P

HEAD = 128
THETA = 10000
NEG = -1e30
HIDDEN = 2 * NEG
LOG2E = 1.4426950408889634
VMEM = 64_400_000
CHUNK = 512
MESH = pl.DeviceIdType.MESH


def _dot(a, b, ca, cb):
    return lax.dot_general(a, b, (((ca,), (cb,)), ((), ())), preferred_element_type=jnp.float32)


def _places(n):
    me = lax.axis_index("tp")
    chips = n // 2
    chip, core = me // 2, me % 2
    right = 2 * ((chip + 1) % chips) + core
    left = 2 * ((chip + chips - 1) % chips) + core
    return chip, core, left, right, 2 * chip + 1 - core


def _greet(devices):
    for d in devices:
        pl.semaphore_signal(pltpu.get_barrier_semaphore(), inc=1, device_id={"tp": d}, device_id_type=MESH)


def _send(src, dst, send_sem, recv_sem, device):
    return pltpu.make_async_remote_copy(src_ref=src, dst_ref=dst, send_sem=send_sem, recv_sem=recv_sem, device_id={"tp": device}, device_id_type=MESH)


def _tables(rows, piece, count):
    half = HEAD // 2
    step = float(THETA) ** (-np.arange(half, dtype=np.float64) / half)

    def pair(place):
        angle = place[:, None] * np.concatenate([step, step])[None, :]
        return np.stack([np.cos(angle), np.sin(angle)]).astype(np.float32)

    return pair(np.arange(piece, dtype=np.float64)), pair(piece * np.arange(count, dtype=np.float64))


def layer(n, x_hbm, gain_hbm, near_hbm, far_hbm, wq_hbm, wk_hbm, wv_hbm, wo_hbm, y_ref, gain_ref, near_ref, far_ref, held, w, wo, q_s, k_s, v_s, seen, top_s, mix_s,
          x_sem, w_sem, send_r, send_l, send_p, recv_r, recv_l, recv_p, give_sem, give_got, sum_r_sem, sum_l_sem, got_l, got_r, y_sem, ready1, ready2, ready3):
    chip, core, left, right, partner = _places(n)
    chips = n // 2
    rows, cols = x_hbm.shape
    heads = q_s.shape[0]
    width = heads * HEAD
    piece, short = rows // 4, rows // 8
    count = cols // CHUNK
    half = count // 2
    e = HEAD**-0.5 * LOG2E
    across, after, before = (chip + 2) % chips, (chip + 1) % chips, (chip + chips - 1) % chips

    x_loads = [pltpu.make_async_copy(x_hbm.at[pl.ds(i * piece, piece)], wo.at[pl.ds(i * piece, piece)], x_sem.at[i]) for i in range(4)]
    smalls = [pltpu.make_async_copy(src, dst, w_sem.at[4 + i]) for i, (src, dst) in enumerate(((gain_hbm, gain_ref), (near_hbm, near_ref), (far_hbm, far_ref)))]
    smalls[0].start()
    x_loads[0].start()
    x_loads[2].start()
    _greet((left, right, partner))
    loads = [pltpu.make_async_copy(src, w.at[:, pl.ds(i * width, width)], w_sem.at[i]) for i, src in enumerate((wk_hbm, wv_hbm, wq_hbm))]
    loads.append(pltpu.make_async_copy(wo_hbm, wo, w_sem.at[3]))


    def at(i):
        return pl.ds(i * piece, piece)

    def lands(s, quarter, quarters=1):
        if isinstance(s, int) and s < 5:
            return held.at[s + 1, :, pl.ds(quarter * piece, quarters * piece)]
        return held.at[6 + (s - 5) // 2, :, pl.ds(pl.multiple_of((s - 5) % 2 * 2 * piece + quarter * short, short), quarters * short)]

    def long_lands(s, quarter, quarters=1):
        return held.at[s + 1, :, pl.ds(quarter * piece, quarters * piece)]

    def to_right(src, s, to=lands):
        return _send(src, to(s, 0), send_r.at[s - 1], recv_l.at[s - 1], right)

    def to_left(src, s, to=lands):
        return _send(src, to(s, 1), send_l.at[s - 1], recv_r.at[s - 1], left)

    def to_partner(s, to=lands):
        if isinstance(s, int) and s == 0:
            return _send(held.at[0], held.at[1], send_p.at[0], recv_p.at[0], partner)
        return _send(to(s, 0, 2), to(s, 2, 2), send_p.at[s], recv_p.at[s], partner)

    def own(i):
        return held.at[0, :, at(i)]

    smalls[0].wait()
    gain = gain_ref[...].astype(jnp.float32).reshape(1, cols)

    def norm(i):
        x_loads[i].wait()
        wide = wo[i * piece : (i + 1) * piece, :].astype(jnp.float32)
        scale = lax.rsqrt(jnp.mean(wide * wide, -1, keepdims=True) + 1e-6)
        a = (wide * scale * gain).astype(jnp.bfloat16)
        for c in range(count):
            held[0, c, i * piece : (i + 1) * piece, :] = a[:, c * CHUNK : (c + 1) * CHUNK]

    norm(0)
    x_loads[1].start()
    x_loads[3].start()
    norm(2)
    pl.semaphore_wait(pltpu.get_barrier_semaphore(), 3)
    to_right(own(0), 1).start()
    norm(1)
    to_left(own(2), 1).start()
    norm(3)
    for load in smalls[1:] + loads:
        load.start()
    to_right(own(1), 2).start()
    to_left(own(3), 2).start()
    to_partner(0).start()
    to_right(own(2), 3).start()
    to_left(own(0), 3).start()
    to_right(own(3), 4).start()
    to_left(own(1), 4).start()
    for load in smalls[1:] + loads[:3]:
        load.wait()

    first_half = lax.broadcasted_iota(jnp.int32, (1, HEAD), 1) < HEAD // 2
    outs = (k_s, v_s, q_s)
    all_heads, keys_values, queries = range(3 * heads), range(2 * heads), range(2 * heads, 3 * heads)

    def project(slot, low, size, starts, which):
        part = size // len(starts)
        turns = []
        for start in starts:
            j = start // piece
            near = pl.ds(pl.multiple_of(start - j * piece, part), part)
            c, s = far_ref[0, pl.ds(j, 1), :], far_ref[1, pl.ds(j, 1), :]
            cn, sn = near_ref[0, near, :], near_ref[1, near, :]
            turns.append((c * cn - s * sn, jnp.where(first_half, -1.0, 1.0) * (s * cn + c * sn)))
        cos = jnp.concatenate([t[0] for t in turns], axis=0)
        sin = jnp.concatenate([t[1] for t in turns], axis=0)
        for h0 in which[::4]:
            got = list(range(h0, min(h0 + 4, which[-1] + 1)))
            a = jnp.concatenate([held[slot, c, pl.ds(low, size), :] for c in range(count)], axis=1)
            t = _dot(a, w[:, h0 * HEAD : (got[-1] + 1) * HEAD], 1, 0).astype(jnp.bfloat16)
            for h in got:
                th = t[:, (h - h0) * HEAD : (h - h0 + 1) * HEAD]
                if h // heads != 1:
                    wide = th.astype(jnp.float32)
                    th = (wide * cos + pltpu.roll(wide, HEAD // 2, 1) * sin).astype(jnp.bfloat16)
                for i, start in enumerate(starts):
                    outs[h // heads][h % heads, pl.ds(pl.multiple_of(start, part), part), :] = th[i * part : (i + 1) * part, :]

    def step(i, _):
        slot, second = i // 2, i % 2
        t = slot - 1

        @pl.when(i == 2)
        def _():
            to_partner(0).wait_recv()

        @pl.when((i >= 4) & (second == 0))
        def _():
            to_right(own(0), t, long_lands).wait_recv()
            to_left(own(0), t, long_lands).wait_recv()
            to_partner(t, long_lands).start()

            @pl.when(t <= 2)
            def _():
                for r in range(2):
                    to_right(held.at[t + 1, :, pl.ds(r * short, short)], 2 * t + 3 + r).start()
                    to_left(held.at[t + 1, :, pl.ds(piece + r * short, short)], 2 * t + 3 + r).start()

        @pl.when((i >= 4) & (second == 1))
        def _():
            to_partner(t, long_lands).wait_recv()

        starts = []
        for r, (from_chip, part) in enumerate(((before, t - 1), (after, (t + 1) % 4))):
            landed_at = (2 * from_chip + jnp.where(second == 0, core, 1 - core)) * rows + part * piece
            whole_at = (2 * chip + jnp.where(i < 2, core, 1 - core)) * rows + (2 * second + r) * piece
            starts.append(jnp.where(i < 4, whole_at, landed_at))
        project(slot, pl.multiple_of(second * 2 * piece, 2 * piece), 2 * piece, starts, all_heads)
        return _

    def short_starts(s):
        return [(2 * across + (core if i < 2 else 1 - core)) * rows + ((s - 5) // 2 + 2 * (i % 2)) * piece + (s - 5) % 2 * short for i in range(4)]

    def hand_over(s):
        to_right(held.at[0, :, pl.ds(0, short)], s).wait_recv()
        to_left(held.at[0, :, pl.ds(0, short)], s).wait_recv()
        to_partner(s).start()


    visible = lax.broadcasted_iota(jnp.int32, (rows, rows), 0) <= lax.broadcasted_iota(jnp.int32, (rows, rows), 1)

    def block(units, keys, sees):
        here = [pl.ds(pl.multiple_of(to * rows, rows), rows) for _, to in units]
        keys = [pl.ds(pl.multiple_of(start, size), size) for start, size in keys]
        ones = jnp.ones((8, sum(k.size for k in keys)), jnp.bfloat16)

        def joined(parts, axis):
            return parts[0] if len(parts) == 1 else jnp.concatenate(parts, axis=axis)

        def take(ref, h, where):
            return joined([ref[h, k, :] for k in where], 0)

        scores = [_dot(take(k_s, h, keys), take(q_s, h, here), 1, 1) for h in range(heads)]
        weights, keeps = [], []
        for h, s in enumerate(scores):
            if sees is not None:
                s = jnp.where(sees, s, HIDDEN)
            old = joined([top_s[u, h : h + 1, :] for u, _ in units], 1)
            top = jnp.maximum(old, s.max(axis=0, keepdims=True))
            for i, (u, _) in enumerate(units):
                top_s[u, h : h + 1, :] = top[:, i * rows : (i + 1) * rows]
            weights.append(jnp.exp2((s - top) * e).astype(jnp.bfloat16))
            keeps.append(jnp.exp2((old - top) * e))
        for h, (p, keep) in enumerate(zip(weights, keeps)):
            mixed = _dot(jnp.concatenate([take(v_s, h, keys).T, ones], axis=0), p, 1, 0)
            for i, (u, _) in enumerate(units):
                part = slice(i * rows, (i + 1) * rows)
                mix_s[u, h] = mix_s[u, h] * keep[:, part] + mixed[:, part]

    def blocks(u, to, low, high):
        def run(j, _):
            block([(u, to)], [(j * rows, rows)], None)
            return _

        lax.fori_loop(low, high, run, None)

    def clear(u):
        top_s[u] = jnp.full(top_s.shape[1:], NEG, jnp.float32)
        mix_s[u] = jnp.zeros(mix_s.shape[1:], jnp.float32)

    def unit(u):
        to_chip = jnp.where(u < 2, after, before)
        return to_chip, 2 * to_chip + jnp.where(u % 2 == 0, 1 - core, core)

    def start_unit(u):
        to_chip, to = unit(u)
        clear(u)
        blocks(u, to, 0, jnp.minimum(2 * across, to))
        blocks(u, to, 2 * across + 2, to)
        block([(u, to)], [(to * rows, rows)], visible)

    def finish(u, slot):
        for h in range(heads):
            o = mix_s[u, h, :HEAD, :] * (1 / mix_s[u, h, HEAD : HEAD + 1, :])
            seen[slot, :, h * HEAD : (h + 1) * HEAD] = o.T.astype(jnp.bfloat16)

    def go_on(u, s):
        (to_chip, a), (_, b) = unit(u), unit(u + 1)

        @pl.when(across < to_chip)
        def _():
            block([(u, a), (u + 1, b)], [(start, short) for start in short_starts(s)], None)

    def attend(to, slot):
        clear(0)
        blocks(0, to, 0, to)
        block([(0, to)], [(to * rows, rows)], visible)
        finish(0, slot)

    lax.fori_loop(0, 12, step, None)

    for u in range(1, 5):
        to_right(own(0), u).wait_send()
        to_left(own(0), u).wait_send()
    for u in range(5):
        to_partner(u).wait_send()
    for d in (left, right, partner):
        pl.semaphore_signal(ready1, inc=1, device_id={"tp": d}, device_id_type=MESH)

    idle = (after < across) & (before < across)
    wait = (after < across) & (before > across)

    def start_units(u, _):
        @pl.when(jnp.logical_not(wait & (u == 1)))
        def _():
            start_unit(u)

        @pl.when(u % 2 == 1)
        def _():
            hand_over(5 + u // 2)

        return _

    lax.fori_loop(0, 4, start_units, None)

    def short_step(s, _):
        to_partner(s).wait_recv()
        low = pl.multiple_of((s - 5) % 2 * 2 * piece, 2 * piece)
        project(6 + (s - 5) // 2, low, 2 * piece, short_starts(s), keys_values)

        @pl.when(s > 5)
        def _():
            hand_over(s + 1)

        lax.fori_loop(0, 2, lambda i, _: go_on(2 * i, s), None)
        return _

    lax.fori_loop(5, 7, short_step, None)
    to_partner(7).wait_recv()
    project(7, 0, 2 * piece, short_starts(7), keys_values)
    lax.fori_loop(0, 2, lambda i, _: go_on(2 * i, 7), None)

    @pl.when(idle)
    def _():
        project(6, 0, rows, short_starts(5) + short_starts(6), queries)

    hand_over(8)

    @pl.when(wait)
    def _():
        start_unit(1)

    @pl.when(jnp.logical_not(idle | wait))
    def _():
        project(6, 0, 2 * piece, short_starts(5), queries)

    to_partner(8).wait_recv()
    project(7, 2 * piece, 2 * piece, short_starts(8), keys_values)


    def columns(j):
        return pl.ds(pl.multiple_of(j * CHUNK, CHUNK), CHUNK)

    def spare(base, j):
        if base < 40:
            i = base + j
            return w.at[pl.ds(pl.multiple_of(i // 2 * rows, rows), rows), columns(i % 2)]
        return w.at[pl.ds(pl.multiple_of((base - 40 + j) * rows, rows), rows), columns(2)]

    right_at, left_at, y_at = (20, 30, 40), (25, 35, 45), 50

    def given(g, j):
        return spare(0, j % half) if g == 1 else spare(half, j % half) if g == 2 else spare(count, j)

    from_p_slots = (3, 0, 1, 6)

    def term(slot, j):
        return _dot(seen[slot], wo[:, columns(j)], 1, 0)

    def give_copy(g, j):
        return _send(given(g, j), held.at[from_p_slots[g], j], give_sem.at[g, j], give_got.at[g, j], partner)

    def ring_slot(base, part, j):
        return held.at[base, part * half + j] if part < 2 else held.at[2, (base - 4) * half + j]

    def right_copy(part, j):
        i = part * half + j
        return _send(spare(right_at[part], j), ring_slot(4, part, j), sum_r_sem.at[i], got_l.at[i], right)

    def left_copy(part, j):
        i = part * half + j
        return _send(spare(left_at[part], j), ring_slot(5, part, j), sum_l_sem.at[i], got_r.at[i], left)

    def landed_l(part, j):
        right_copy(part, j).wait_recv()
        return ring_slot(4, part, j)[...].astype(jnp.float32)

    def landed_r(part, j):
        left_copy(part, j).wait_recv()
        return ring_slot(5, part, j)[...].astype(jnp.float32)

    def give(*which):
        terms = [term(slot, j).astype(jnp.bfloat16) for g, slot, j, _ in which]
        for (g, slot, j, old), t in zip(which, terms):
            if old is not None:
                give_copy(*old).wait_send()
            given(g, j)[...] = t
        for g, slot, j, _ in which:
            give_copy(g, j).start()

    def pairs(*which):
        terms = [term(slot, j) for g, slot, j in which]
        for g, slot, j in which:
            give_copy(g, j).wait_recv()
        return [t + held[from_p_slots[g], j].astype(jnp.float32) for (g, slot, j), t in zip(which, terms)]

    def emit(part, j, rightwards, leftwards):
        spare(right_at[part], j)[...] = rightwards.astype(jnp.bfloat16)
        spare(left_at[part], j)[...] = leftwards.astype(jnp.bfloat16)
        right_copy(part, j).start()
        left_copy(part, j).start()

    def loop(body):
        def run(j, _):
            body(j)
            return _

        lax.fori_loop(0, half, run, None)

    x_again = [pltpu.make_async_copy(x_hbm.at[:, columns(j)], held.at[7, j], x_sem.at[4 + j]) for j in range(count)]

    def begin(j):
        give((1, 0, half + j, None), (2, 2, j, None))

    def part0(j):
        emit(0, j, *pairs((1, 1, half + j), (2, 3, j)))

        @pl.when(j < half - 1)
        def _():
            begin(j + 1)

    go_on(0, 8)
    go_on(2, 8)
    finish(0, 0)
    finish(2, 2)
    loads[3].wait()
    pl.semaphore_wait(ready1, 3)
    begin(0)
    finish(1, 1)
    finish(3, 3)
    for s in range(5, 9):
        to_right(held.at[0, :, pl.ds(0, short)], s).wait_send()
        to_left(held.at[0, :, pl.ds(0, short)], s).wait_send()
    for d in (left, right, partner):
        pl.semaphore_signal(ready2, inc=1, device_id={"tp": d}, device_id_type=MESH)
    loop(part0)

    @pl.when(wait)
    def _():
        project(6, 0, 2 * piece, short_starts(5), queries)

    @pl.when(jnp.logical_not(idle))
    def _():
        project(6, 2 * piece, 2 * piece, short_starts(6), queries)

    project(7, 0, rows, short_starts(7) + short_starts(8), queries)
    for s in range(5, 9):
        to_partner(s).wait_send()
    pl.semaphore_signal(ready3, inc=1, device_id={"tp": partner}, device_id_type=MESH)
    for load in x_again:
        load.start()
    attend(2 * across + 1 - core, 4)
    pl.semaphore_wait(ready2, 3)
    loop(lambda j: give((0, 4, j, None), (0, 4, half + j, None)))
    attend(2 * across + core, 4)
    loop(lambda j: emit(1, j, *pairs((0, 4, j), (0, 4, half + j))))

    loop(lambda j: give((1, 0, j, (1, half + j)), (2, 2, half + j, (2, j))))
    attend(2 * chip + 1 - core, 4)
    pl.semaphore_wait(ready3, 1)
    loop(lambda j: give((3, 4, j, (0, j)), (3, 4, half + j, (0, half + j))))
    attend(2 * chip + core, 4)

    def part2(j):
        a, b = pairs((1, 1, j), (2, 3, half + j))
        emit(2, j, a + landed_l(1, j), b + landed_r(1, j))

    loop(part2)

    def y_copy(j):
        return pltpu.make_async_copy(spare(y_at, j), y_ref.at[:, columns(j)], y_sem.at[j])

    def last(j):
        a, b = pairs((3, 4, j), (3, 4, half + j))
        a += held[7, j].astype(jnp.float32)
        b += held[7, half + j].astype(jnp.float32)
        spare(y_at, j)[...] = (a + landed_r(0, j) + landed_l(2, j)).astype(jnp.bfloat16)
        y_copy(j).start()
        spare(y_at, half + j)[...] = (b + landed_l(0, j) + landed_r(2, j)).astype(jnp.bfloat16)
        y_copy(half + j).start()

    for load in x_again:
        load.wait()
    loop(last)

    def drain(j):
        for copy in (give_copy(1, j), give_copy(2, half + j), give_copy(3, j), give_copy(3, half + j)):
            copy.wait_send()
        for part in range(3):
            right_copy(part, j).wait_send()
            left_copy(part, j).wait_send()
        y_copy(j).wait()
        y_copy(half + j).wait()

    loop(drain)


def solution(mesh):
    n = mesh.shape["tp"]

    def step(x, gain, wq, wk, wv, wo):
        rows, cols = x.shape
        width = wq.shape[1]
        heads = width // HEAD
        tokens = n * rows
        count = cols // CHUNK
        ring = 3 * (count // 2)
        near, far = _tables(rows, rows // 4, tokens // (rows // 4))
        hbm = pl.BlockSpec(memory_space=pl.ANY)
        dma = pltpu.SemaphoreType.DMA
        low = jnp.bfloat16
        return pl.pallas_call(
            functools.partial(layer, n),
            name="layer",
            out_shape=pltpu.VMEM((rows, cols), low),
            in_specs=[hbm] * 8,
            out_specs=hbm,
            scratch_shapes=[
                pltpu.VMEM((cols,), low),
                pltpu.VMEM(near.shape, jnp.float32),
                pltpu.VMEM(far.shape, jnp.float32),
                pltpu.VMEM((8, count, rows, CHUNK), low),
                pltpu.VMEM((cols, 3 * width), low),
                pltpu.VMEM((width, cols), low),
                *[pltpu.VMEM((heads, tokens, HEAD), low)] * 3,
                pltpu.VMEM((5, rows, width), low),
                pltpu.VMEM((4, heads, rows), jnp.float32),
                pltpu.VMEM((4, heads, HEAD + 8, rows), jnp.float32),
                dma((4 + count,)), dma((7,)), dma((8,)), dma((8,)), dma((9,)), dma((8,)), dma((8,)), dma((9,)),
                dma((4, count)), dma((4, count)), dma((ring,)), dma((ring,)), dma((ring,)), dma((ring,)), dma((count,)),
                *[pltpu.SemaphoreType.REGULAR] * 3,
            ],
            compiler_params=pltpu.CompilerParams(collective_id=0, has_side_effects=True, vmem_limit_bytes=VMEM),
        )(x, gain, jnp.asarray(near), jnp.asarray(far), wq, wk, wv, wo)

    tokens, columns = P(("dp", "tp"), None), P(None, "tp")
    return jax.shard_map(
        step,
        mesh=mesh,
        in_specs=(tokens, P(None), columns, columns, columns, P("tp", None)),
        out_specs=tokens,
        check_vma=False,
    )
```

```python
import functools

import jax
import jax.numpy as jnp
import numpy as np
from jax import lax
from jax.experimental import pallas as pl
from jax.experimental.pallas import tpu as pltpu
from jax.sharding import PartitionSpec as P

HEAD = 128
THETA = 10000
NEG = -1e30
HIDDEN = 2 * NEG
LOG2E = 1.4426950408889634
VMEM = 64_400_000
CHUNK = 512
MESH = pl.DeviceIdType.MESH


def _dot(a, b, ca, cb):
    return lax.dot_general(a, b, (((ca,), (cb,)), ((), ())), preferred_element_type=jnp.float32)


def _places(n):
    me = lax.axis_index("tp")
    chips = n // 2
    chip, core = me // 2, me % 2
    right = 2 * ((chip + 1) % chips) + core
    left = 2 * ((chip + chips - 1) % chips) + core
    return chip, core, left, right, 2 * chip + 1 - core


def _greet(devices):
    for d in devices:
        pl.semaphore_signal(pltpu.get_barrier_semaphore(), inc=1, device_id={"tp": d}, device_id_type=MESH)


def _send(src, dst, send_sem, recv_sem, device):
    return pltpu.make_async_remote_copy(src_ref=src, dst_ref=dst, send_sem=send_sem, recv_sem=recv_sem, device_id={"tp": device}, device_id_type=MESH)


def _tables(rows, piece, count):
    half = HEAD // 2
    step = float(THETA) ** (-np.arange(half, dtype=np.float64) / half)

    def pair(place):
        angle = place[:, None] * np.concatenate([step, step])[None, :]
        return np.stack([np.cos(angle), np.sin(angle)]).astype(np.float32)

    return pair(np.arange(piece, dtype=np.float64)), pair(piece * np.arange(count, dtype=np.float64))


def layer(n, x_hbm, gain_hbm, near_hbm, far_hbm, wq_hbm, wk_hbm, wv_hbm, wo_hbm, y_ref, gain_ref, near_ref, far_ref, held, w, wo, q_s, k_s, v_s, seen, top_s, mix_s,
          x_sem, w_sem, send_r, send_l, send_p, recv_r, recv_l, recv_p, give_sem, give_got, sum_r_sem, sum_l_sem, got_l, got_r, y_sem, ready1, ready2, ready3):
    chip, core, left, right, partner = _places(n)
    chips = n // 2
    rows, cols = x_hbm.shape
    heads = q_s.shape[0]
    width = heads * HEAD
    piece, short = rows // 4, rows // 8
    count = cols // CHUNK
    half = count // 2
    e = HEAD**-0.5 * LOG2E
    across, after, before = (chip + 2) % chips, (chip + 1) % chips, (chip + chips - 1) % chips

    x_loads = [pltpu.make_async_copy(x_hbm.at[pl.ds(i * piece, piece)], wo.at[pl.ds(i * piece, piece)], x_sem.at[i]) for i in range(4)]
    smalls = [pltpu.make_async_copy(src, dst, w_sem.at[4 + i]) for i, (src, dst) in enumerate(((gain_hbm, gain_ref), (near_hbm, near_ref), (far_hbm, far_ref)))]
    smalls[0].start()
    x_loads[0].start()
    x_loads[2].start()
    _greet((left, right, partner))
    loads = [pltpu.make_async_copy(src, w.at[:, pl.ds(i * width, width)], w_sem.at[i]) for i, src in enumerate((wk_hbm, wv_hbm, wq_hbm))]
    loads.append(pltpu.make_async_copy(wo_hbm, wo, w_sem.at[3]))


    def at(i):
        return pl.ds(i * piece, piece)

    def lands(s, quarter, quarters=1):
        if isinstance(s, int) and s < 5:
            return held.at[s + 1, :, pl.ds(quarter * piece, quarters * piece)]
        return held.at[6 + (s - 5) // 2, :, pl.ds(pl.multiple_of((s - 5) % 2 * 2 * piece + quarter * short, short), quarters * short)]

    def long_lands(s, quarter, quarters=1):
        return held.at[s + 1, :, pl.ds(quarter * piece, quarters * piece)]

    def to_right(src, s, to=lands):
        return _send(src, to(s, 0), send_r.at[s - 1], recv_l.at[s - 1], right)

    def to_left(src, s, to=lands):
        return _send(src, to(s, 1), send_l.at[s - 1], recv_r.at[s - 1], left)

    def to_partner(s, to=lands):
        if isinstance(s, int) and s == 0:
            return _send(held.at[0], held.at[1], send_p.at[0], recv_p.at[0], partner)
        return _send(to(s, 0, 2), to(s, 2, 2), send_p.at[s], recv_p.at[s], partner)

    def own(i):
        return held.at[0, :, at(i)]

    smalls[0].wait()
    gain = gain_ref[...].astype(jnp.float32).reshape(1, cols)

    def norm(i):
        x_loads[i].wait()
        wide = wo[i * piece : (i + 1) * piece, :].astype(jnp.float32)
        scale = lax.rsqrt(jnp.mean(wide * wide, -1, keepdims=True) + 1e-6)
        a = (wide * scale * gain).astype(jnp.bfloat16)
        for c in range(count):
            held[0, c, i * piece : (i + 1) * piece, :] = a[:, c * CHUNK : (c + 1) * CHUNK]

    norm(0)
    x_loads[1].start()
    x_loads[3].start()
    norm(2)
    pl.semaphore_wait(pltpu.get_barrier_semaphore(), 3)
    to_right(own(0), 1).start()
    norm(1)
    to_left(own(2), 1).start()
    norm(3)
    for load in smalls[1:] + loads:
        load.start()
    to_right(own(1), 2).start()
    to_left(own(3), 2).start()
    to_partner(0).start()
    to_right(own(2), 3).start()
    to_left(own(0), 3).start()
    to_right(own(3), 4).start()
    to_left(own(1), 4).start()
    for load in smalls[1:] + loads[:3]:
        load.wait()

    first_half = lax.broadcasted_iota(jnp.int32, (1, HEAD), 1) < HEAD // 2
    outs = (k_s, v_s, q_s)
    all_heads, keys_values, queries = range(3 * heads), range(2 * heads), range(2 * heads, 3 * heads)

    def project(slot, low, size, starts, which):
        part = size // len(starts)
        turns = []
        for start in starts:
            j = start // piece
            near = pl.ds(pl.multiple_of(start - j * piece, part), part)
            c, s = far_ref[0, pl.ds(j, 1), :], far_ref[1, pl.ds(j, 1), :]
            cn, sn = near_ref[0, near, :], near_ref[1, near, :]
            turns.append((c * cn - s * sn, jnp.where(first_half, -1.0, 1.0) * (s * cn + c * sn)))
        cos = jnp.concatenate([t[0] for t in turns], axis=0)
        sin = jnp.concatenate([t[1] for t in turns], axis=0)
        for h0 in which[::4]:
            got = list(range(h0, min(h0 + 4, which[-1] + 1)))
            a = jnp.concatenate([held[slot, c, pl.ds(low, size), :] for c in range(count)], axis=1)
            t = _dot(a, w[:, h0 * HEAD : (got[-1] + 1) * HEAD], 1, 0).astype(jnp.bfloat16)
            for h in got:
                th = t[:, (h - h0) * HEAD : (h - h0 + 1) * HEAD]
                if h // heads != 1:
                    wide = th.astype(jnp.float32)
                    th = (wide * cos + pltpu.roll(wide, HEAD // 2, 1) * sin).astype(jnp.bfloat16)
                for i, start in enumerate(starts):
                    outs[h // heads][h % heads, pl.ds(pl.multiple_of(start, part), part), :] = th[i * part : (i + 1) * part, :]

    def step(i, _):
        slot, second = i // 2, i % 2
        t = slot - 1

        @pl.when(i == 2)
        def _():
            to_partner(0).wait_recv()

        @pl.when((i >= 4) & (second == 0))
        def _():
            to_right(own(0), t, long_lands).wait_recv()
            to_left(own(0), t, long_lands).wait_recv()
            to_partner(t, long_lands).start()

            @pl.when(t <= 2)
            def _():
                for r in range(2):
                    to_right(held.at[t + 1, :, pl.ds(r * short, short)], 2 * t + 3 + r).start()
                    to_left(held.at[t + 1, :, pl.ds(piece + r * short, short)], 2 * t + 3 + r).start()

        @pl.when((i >= 4) & (second == 1))
        def _():
            to_partner(t, long_lands).wait_recv()

        starts = []
        for r, (from_chip, part) in enumerate(((before, t - 1), (after, (t + 1) % 4))):
            landed_at = (2 * from_chip + jnp.where(second == 0, core, 1 - core)) * rows + part * piece
            whole_at = (2 * chip + jnp.where(i < 2, core, 1 - core)) * rows + (2 * second + r) * piece
            starts.append(jnp.where(i < 4, whole_at, landed_at))
        project(slot, pl.multiple_of(second * 2 * piece, 2 * piece), 2 * piece, starts, all_heads)
        return _

    def short_starts(s):
        return [(2 * across + (core if i < 2 else 1 - core)) * rows + ((s - 5) // 2 + 2 * (i % 2)) * piece + (s - 5) % 2 * short for i in range(4)]

    def hand_over(s):
        to_right(held.at[0, :, pl.ds(0, short)], s).wait_recv()
        to_left(held.at[0, :, pl.ds(0, short)], s).wait_recv()
        to_partner(s).start()


    visible = lax.broadcasted_iota(jnp.int32, (rows, rows), 0) <= lax.broadcasted_iota(jnp.int32, (rows, rows), 1)

    def block(units, keys, sees):
        here = [pl.ds(pl.multiple_of(to * rows, rows), rows) for _, to in units]
        keys = [pl.ds(pl.multiple_of(start, size), size) for start, size in keys]
        ones = jnp.ones((8, sum(k.size for k in keys)), jnp.bfloat16)

        def joined(parts, axis):
            return parts[0] if len(parts) == 1 else jnp.concatenate(parts, axis=axis)

        def take(ref, h, where):
            return joined([ref[h, k, :] for k in where], 0)

        scores = [_dot(take(k_s, h, keys), take(q_s, h, here), 1, 1) for h in range(heads)]
        weights, keeps = [], []
        for h, s in enumerate(scores):
            if sees is not None:
                s = jnp.where(sees, s, HIDDEN)
            old = joined([top_s[u, h : h + 1, :] for u, _ in units], 1)
            top = jnp.maximum(old, s.max(axis=0, keepdims=True))
            for i, (u, _) in enumerate(units):
                top_s[u, h : h + 1, :] = top[:, i * rows : (i + 1) * rows]
            weights.append(jnp.exp2((s - top) * e).astype(jnp.bfloat16))
            keeps.append(jnp.exp2((old - top) * e))
        for h, (p, keep) in enumerate(zip(weights, keeps)):
            mixed = _dot(jnp.concatenate([take(v_s, h, keys).T, ones], axis=0), p, 1, 0)
            for i, (u, _) in enumerate(units):
                part = slice(i * rows, (i + 1) * rows)
                mix_s[u, h] = mix_s[u, h] * keep[:, part] + mixed[:, part]

    def blocks(u, to, low, high):
        def run(j, _):
            block([(u, to)], [(j * rows, rows)], None)
            return _

        lax.fori_loop(low, high, run, None)

    def clear(u):
        top_s[u] = jnp.full(top_s.shape[1:], NEG, jnp.float32)
        mix_s[u] = jnp.zeros(mix_s.shape[1:], jnp.float32)

    def unit(u):
        to_chip = jnp.where(u < 2, after, before)
        return to_chip, 2 * to_chip + jnp.where(u % 2 == 0, 1 - core, core)

    def start_unit(u):
        to_chip, to = unit(u)
        clear(u)
        blocks(u, to, 0, jnp.minimum(2 * across, to))
        blocks(u, to, 2 * across + 2, to)
        block([(u, to)], [(to * rows, rows)], visible)

    def finish(u, slot):
        for h in range(heads):
            o = mix_s[u, h, :HEAD, :] * (1 / mix_s[u, h, HEAD : HEAD + 1, :])
            seen[slot, :, h * HEAD : (h + 1) * HEAD] = o.T.astype(jnp.bfloat16)

    def go_on(u, s):
        (to_chip, a), (_, b) = unit(u), unit(u + 1)

        @pl.when(across < to_chip)
        def _():
            block([(u, a), (u + 1, b)], [(start, short) for start in short_starts(s)], None)

    def attend(to, slot):
        clear(0)
        blocks(0, to, 0, to)
        block([(0, to)], [(to * rows, rows)], visible)
        finish(0, slot)

    lax.fori_loop(0, 12, step, None)

    for u in range(1, 5):
        to_right(own(0), u).wait_send()
        to_left(own(0), u).wait_send()
    for u in range(5):
        to_partner(u).wait_send()
    for d in (left, right, partner):
        pl.semaphore_signal(ready1, inc=1, device_id={"tp": d}, device_id_type=MESH)

    idle = (after < across) & (before < across)
    wait = (after < across) & (before > across)

    def start_units(u, _):
        @pl.when(jnp.logical_not(wait & (u == 1)))
        def _():
            start_unit(u)

        @pl.when(u % 2 == 1)
        def _():
            hand_over(5 + u // 2)

        return _

    lax.fori_loop(0, 4, start_units, None)

    def short_step(s, _):
        to_partner(s).wait_recv()
        low = pl.multiple_of((s - 5) % 2 * 2 * piece, 2 * piece)
        project(6 + (s - 5) // 2, low, 2 * piece, short_starts(s), keys_values)

        @pl.when(s > 5)
        def _():
            hand_over(s + 1)

        lax.fori_loop(0, 2, lambda i, _: go_on(2 * i, s), None)
        return _

    lax.fori_loop(5, 7, short_step, None)
    to_partner(7).wait_recv()
    project(7, 0, 2 * piece, short_starts(7), keys_values)
    lax.fori_loop(0, 2, lambda i, _: go_on(2 * i, 7), None)

    @pl.when(idle)
    def _():
        project(6, 0, rows, short_starts(5) + short_starts(6), queries)

    last_pair = [_send(lands(8, i), lands(8, 2 + i), send_p.at[8 + i], recv_p.at[8 + i], partner) for i in range(2)]
    to_right(held.at[0, :, pl.ds(0, short)], 8).wait_recv()
    last_pair[0].start()
    to_left(held.at[0, :, pl.ds(0, short)], 8).wait_recv()
    last_pair[1].start()

    @pl.when(wait)
    def _():
        start_unit(1)

    @pl.when(jnp.logical_not(idle | wait))
    def _():
        project(6, 0, 2 * piece, short_starts(5), queries)

    for copy in last_pair:
        copy.wait_recv()
    project(7, 2 * piece, 2 * piece, short_starts(8), keys_values)


    def columns(j):
        return pl.ds(pl.multiple_of(j * CHUNK, CHUNK), CHUNK)

    def spare(base, j):
        if base < 40:
            i = base + j
            return w.at[pl.ds(pl.multiple_of(i // 2 * rows, rows), rows), columns(i % 2)]
        return w.at[pl.ds(pl.multiple_of((base - 40 + j) * rows, rows), rows), columns(2)]

    right_at, left_at, y_at = (20, 30, 40), (25, 35, 45), 50

    def given(g, j):
        return spare(0, j % half) if g == 1 else spare(half, j % half) if g == 2 else spare(count, j)

    from_p_slots = (3, 0, 1, 6)

    def term(slot, j):
        return _dot(seen[slot], wo[:, columns(j)], 1, 0)

    def give_copy(g, j):
        return _send(given(g, j), held.at[from_p_slots[g], j], give_sem.at[g, j], give_got.at[g, j], partner)

    def ring_slot(base, part, j):
        return held.at[base, part * half + j] if part < 2 else held.at[2, (base - 4) * half + j]

    def right_copy(part, j):
        i = part * half + j
        return _send(spare(right_at[part], j), ring_slot(4, part, j), sum_r_sem.at[i], got_l.at[i], right)

    def left_copy(part, j):
        i = part * half + j
        return _send(spare(left_at[part], j), ring_slot(5, part, j), sum_l_sem.at[i], got_r.at[i], left)

    def landed_l(part, j):
        right_copy(part, j).wait_recv()
        return ring_slot(4, part, j)[...].astype(jnp.float32)

    def landed_r(part, j):
        left_copy(part, j).wait_recv()
        return ring_slot(5, part, j)[...].astype(jnp.float32)

    def give(*which):
        terms = [term(slot, j).astype(jnp.bfloat16) for g, slot, j, _ in which]
        for (g, slot, j, old), t in zip(which, terms):
            if old is not None:
                give_copy(*old).wait_send()
            given(g, j)[...] = t
        for g, slot, j, _ in which:
            give_copy(g, j).start()

    def pairs(*which):
        terms = [term(slot, j) for g, slot, j in which]
        for g, slot, j in which:
            give_copy(g, j).wait_recv()
        return [t + held[from_p_slots[g], j].astype(jnp.float32) for (g, slot, j), t in zip(which, terms)]

    def emit(part, j, rightwards, leftwards):
        spare(right_at[part], j)[...] = rightwards.astype(jnp.bfloat16)
        spare(left_at[part], j)[...] = leftwards.astype(jnp.bfloat16)
        right_copy(part, j).start()
        left_copy(part, j).start()

    def loop(body):
        def run(j, _):
            body(j)
            return _

        lax.fori_loop(0, half, run, None)

    x_again = [pltpu.make_async_copy(x_hbm.at[:, columns(j)], held.at[7, j], x_sem.at[4 + j]) for j in range(count)]

    def begin(j):
        give((1, 0, half + j, None), (2, 2, j, None))

    def part0(j):
        emit(0, j, *pairs((1, 1, half + j), (2, 3, j)))

        @pl.when(j < half - 1)
        def _():
            begin(j + 1)

    go_on(0, 8)
    go_on(2, 8)
    finish(0, 0)
    finish(2, 2)
    loads[3].wait()
    pl.semaphore_wait(ready1, 3)
    begin(0)
    finish(1, 1)
    finish(3, 3)
    for s in range(5, 9):
        to_right(held.at[0, :, pl.ds(0, short)], s).wait_send()
        to_left(held.at[0, :, pl.ds(0, short)], s).wait_send()
    for d in (left, right, partner):
        pl.semaphore_signal(ready2, inc=1, device_id={"tp": d}, device_id_type=MESH)
    loop(part0)

    @pl.when(wait)
    def _():
        project(6, 0, 2 * piece, short_starts(5), queries)

    @pl.when(jnp.logical_not(idle))
    def _():
        project(6, 2 * piece, 2 * piece, short_starts(6), queries)

    project(7, 0, rows, short_starts(7) + short_starts(8), queries)
    for s in range(5, 8):
        to_partner(s).wait_send()
    for copy in last_pair:
        copy.wait_send()
    pl.semaphore_signal(ready3, inc=1, device_id={"tp": partner}, device_id_type=MESH)
    for load in x_again:
        load.start()
    attend(2 * across + 1 - core, 4)
    pl.semaphore_wait(ready2, 3)
    loop(lambda j: give((0, 4, j, None), (0, 4, half + j, None)))
    attend(2 * across + core, 4)
    loop(lambda j: emit(1, j, *pairs((0, 4, j), (0, 4, half + j))))

    loop(lambda j: give((1, 0, j, (1, half + j)), (2, 2, half + j, (2, j))))
    attend(2 * chip + 1 - core, 4)
    pl.semaphore_wait(ready3, 1)
    loop(lambda j: give((3, 4, j, (0, j)), (3, 4, half + j, (0, half + j))))
    attend(2 * chip + core, 4)

    def part2(j):
        a, b = pairs((1, 1, j), (2, 3, half + j))
        emit(2, j, a + landed_l(1, j), b + landed_r(1, j))

    loop(part2)

    def y_copy(j):
        return pltpu.make_async_copy(spare(y_at, j), y_ref.at[:, columns(j)], y_sem.at[j])

    def last(j):
        a, b = pairs((3, 4, j), (3, 4, half + j))
        a += held[7, j].astype(jnp.float32)
        b += held[7, half + j].astype(jnp.float32)
        spare(y_at, j)[...] = (a + landed_r(0, j) + landed_l(2, j)).astype(jnp.bfloat16)
        y_copy(j).start()
        spare(y_at, half + j)[...] = (b + landed_l(0, j) + landed_r(2, j)).astype(jnp.bfloat16)
        y_copy(half + j).start()

    for load in x_again:
        load.wait()
    loop(last)

    def drain(j):
        for copy in (give_copy(1, j), give_copy(2, half + j), give_copy(3, j), give_copy(3, half + j)):
            copy.wait_send()
        for part in range(3):
            right_copy(part, j).wait_send()
            left_copy(part, j).wait_send()
        y_copy(j).wait()
        y_copy(half + j).wait()

    loop(drain)


def solution(mesh):
    n = mesh.shape["tp"]

    def step(x, gain, wq, wk, wv, wo):
        rows, cols = x.shape
        width = wq.shape[1]
        heads = width // HEAD
        tokens = n * rows
        count = cols // CHUNK
        ring = 3 * (count // 2)
        near, far = _tables(rows, rows // 4, tokens // (rows // 4))
        hbm = pl.BlockSpec(memory_space=pl.ANY)
        dma = pltpu.SemaphoreType.DMA
        low = jnp.bfloat16
        return pl.pallas_call(
            functools.partial(layer, n),
            name="layer",
            out_shape=pltpu.VMEM((rows, cols), low),
            in_specs=[hbm] * 8,
            out_specs=hbm,
            scratch_shapes=[
                pltpu.VMEM((cols,), low),
                pltpu.VMEM(near.shape, jnp.float32),
                pltpu.VMEM(far.shape, jnp.float32),
                pltpu.VMEM((8, count, rows, CHUNK), low),
                pltpu.VMEM((cols, 3 * width), low),
                pltpu.VMEM((width, cols), low),
                *[pltpu.VMEM((heads, tokens, HEAD), low)] * 3,
                pltpu.VMEM((5, rows, width), low),
                pltpu.VMEM((4, heads, rows), jnp.float32),
                pltpu.VMEM((4, heads, HEAD + 8, rows), jnp.float32),
                dma((4 + count,)), dma((7,)), dma((8,)), dma((8,)), dma((10,)), dma((8,)), dma((8,)), dma((10,)),
                dma((4, count)), dma((4, count)), dma((ring,)), dma((ring,)), dma((ring,)), dma((ring,)), dma((count,)),
                *[pltpu.SemaphoreType.REGULAR] * 3,
            ],
            compiler_params=pltpu.CompilerParams(collective_id=0, has_side_effects=True, vmem_limit_bytes=VMEM),
        )(x, gain, jnp.asarray(near), jnp.asarray(far), wq, wk, wv, wo)

    tokens, columns = P(("dp", "tp"), None), P(None, "tp")
    return jax.shard_map(
        step,
        mesh=mesh,
        in_specs=(tokens, P(None), columns, columns, columns, P("tp", None)),
        out_specs=tokens,
        check_vma=False,
    )
```
